8 devices in a mesh: dp: 1 (over z), sp: 8 (over x, y, core).
Axes of the slice: x: 2, y: 2, z: 1, core: 2. Of those that a mesh axis runs over, the one named last changes fastest.
Arguments:
- x: bfloat16 [8192, 2048], P(('dp', 'sp'))
- gain: bfloat16 [2048], replicated
- wq: bfloat16 [2048, 2048], P('sp')
- wk: bfloat16 [2048, 2048], P('sp')
- wv: bfloat16 [2048, 2048], P('sp')
- wo: bfloat16 [2048, 2048], P('sp')
Outputs:
- output: bfloat16 [8192, 2048], P(('dp', 'sp'))
All inputs are finite; a program needn't handle non-finite values.
Results may differ from the reference program's by a relative error of at most 0.012.
Values are sent between devices in bfloat16 or wider.
A program may use at most 2 GiB of HBM per device.

```python
import jax
import jax.numpy as jnp
from jax import lax

ROWS = 8192
D = 2048
HEADS = 8
KV_HEADS = 8
HEAD = 256
THETA = 10000


def setup_inputs(seed: int = 0, part: int = 0) -> dict:
    kx, kn, kq, kk, kv, ko = jax.random.split(jax.random.key(seed), 6)

    def weights(key, rows, columns):
        return jax.random.normal(key, (rows, columns), jnp.float32) * rows**-0.5

    drawn = {
        "x": jax.random.normal(jax.random.fold_in(kx, part), (ROWS, D), jnp.float32),
        "gain": 1 + 0.1 * jax.random.normal(kn, (D,), jnp.float32),
        "wq": 2 * weights(kq, D, HEADS * HEAD),
        "wk": 2 * weights(kk, D, KV_HEADS * HEAD),
        "wv": 4 * weights(kv, D, KV_HEADS * HEAD),
        "wo": weights(ko, HEADS * HEAD, D),
    }
    return {k: v.astype(jnp.bfloat16) for k, v in drawn.items()}


def normed(x, gain):
    wide = x.astype(jnp.float32)
    scale = lax.rsqrt(jnp.mean(wide * wide, -1, keepdims=True) + 1e-6)
    return (wide * scale * gain.astype(jnp.float32)).astype(jnp.bfloat16)


def turned(t, place, theta):
    half = t.shape[-1] // 2
    angle = place.astype(jnp.float32)[:, None] * theta ** (-jnp.arange(half, dtype=jnp.float32) / half)
    cos, sin = jnp.cos(angle)[:, None], jnp.sin(angle)[:, None]
    a, b = t[..., :half].astype(jnp.float32), t[..., half:].astype(jnp.float32)
    return jnp.concatenate([a * cos - b * sin, b * cos + a * sin], -1).astype(jnp.bfloat16)


def matmul(a, w):
    return jnp.dot(a, w, preferred_element_type=jnp.float32).astype(jnp.bfloat16)


def einsum(form, a, b):
    return jnp.einsum(form, a.astype(jnp.float32), b.astype(jnp.float32))


def attention(q, k, v):
    scores = einsum("tgsd,ugd->gstu", q, k) * q.shape[-1] ** -0.5
    token = jnp.arange(q.shape[0])
    scores = jnp.where(token[:, None] >= token, scores, -jnp.inf)
    weights = jax.nn.softmax(scores, -1).astype(jnp.bfloat16)
    return einsum("gstu,ugd->tgsd", weights, v).astype(jnp.bfloat16)


def reference(x, gain, wq, wk, wv, wo):
    a, place = normed(x, gain), jnp.arange(ROWS)
    q = turned(matmul(a, wq).reshape(ROWS, HEADS, HEAD), place, THETA).reshape(ROWS, KV_HEADS, -1, HEAD)
    k = turned(matmul(a, wk).reshape(ROWS, KV_HEADS, HEAD), place, THETA)
    v = matmul(a, wv).reshape(ROWS, KV_HEADS, HEAD)
    seen = attention(q, k, v).reshape(ROWS, HEADS * HEAD)
    return (x.astype(jnp.float32) + jnp.dot(seen, wo, preferred_element_type=jnp.float32)).astype(jnp.bfloat16)
```

```python
import functools

import jax
import jax.numpy as jnp
from jax import lax
from jax.experimental import pallas as pl
from jax.experimental.pallas import tpu as pltpu
from jax.sharding import PartitionSpec as P

NEG = -1e30
LOG2E = 1.4426950408889634
HEAD = 256
THETA = 10000
VMEM = 56 * 2**20
STRIP = 512
KEYS = 512
CHUNK = 2048


def _first(d):
    return d ^ (4 - 2 * (d & 1))


def _second(d):
    return d ^ (2 + 2 * (d & 1))


RELATIONS = (
    (lambda d: d, lambda d: d),
    (lambda d: d ^ 1, lambda d: d ^ 1),
    (_first, _first),
    (_second, _second),
    (lambda d: d ^ 6, lambda d: d ^ 6),
    (lambda d: _first(d ^ 1), lambda d: _first(d) ^ 1),
    (lambda d: _second(d ^ 1), lambda d: _second(d) ^ 1),
    (lambda d: d ^ 7, lambda d: d ^ 7),
)


def permute(t, relation):
    source = RELATIONS[relation][0]
    return lax.ppermute(t, "sp", [(source(d), d) for d in range(8)])


def gathered(t):
    first = permute(t, 2)
    t, first = lax.optimization_barrier((t, first))
    second = permute(t, 3)
    diagonal = permute(first, 3)
    return [t, permute(t, 1), first, second, diagonal, permute(first, 1), permute(second, 1), permute(diagonal, 1)]


def exchanged(block, me, *after):
    blocks = [block(target(me)) for _, target in RELATIONS]
    *blocks, = lax.optimization_barrier((*blocks, *after))
    return [blocks[0]] + [permute(blocks[r], r) for r in range(1, 8)], *blocks[8:]


def normed(x, gain):
    wide = x.astype(jnp.float32)
    scale = lax.rsqrt(jnp.mean(wide * wide, -1, keepdims=True) + 1e-6)
    return (wide * scale * gain.astype(jnp.float32)).astype(jnp.bfloat16)


def _dot(a, b, ca, cb):
    return lax.dot_general(a, b, (((ca,), (cb,)), ((), ())), preferred_element_type=jnp.float32)


def _project(at_ref, a_ref, cos_ref, sin_ref, *rest):
    w_refs, (q_ref, k_ref, v_ref) = rest[:8], rest[-3:]
    total = None
    for n, w_ref in enumerate(w_refs):
        columns = pl.ds(pl.multiple_of(at_ref[1 + n] * HEAD, HEAD), HEAD)
        part = _dot(a_ref[:, columns], w_ref[...], 1, 0)
        total = part if total is None else total + part
    total = total.astype(jnp.bfloat16)
    cos, sin = cos_ref[...], sin_ref[...]
    half = HEAD // 2
    for ref, at in ((q_ref, 0), (k_ref, HEAD)):
        first, second = total[:, at : at + half].astype(jnp.float32), total[:, at + half : at + HEAD].astype(jnp.float32)
        ref[:, :half] = (first * cos - second * sin).astype(jnp.bfloat16)
        ref[:, half:] = (second * cos + first * sin).astype(jnp.bfloat16)
    v_ref[...] = total[:, 2 * HEAD :]


def project(piece, w, order, a, cos, sin, so_far):
    tokens, depth = a.shape
    tile = 512
    per = tokens // tile
    everything = 8 * tokens
    at = jnp.stack([piece, *order]).astype(jnp.int32)
    place = lambda i, at_ref: (at_ref[0] * per + i, 0)
    given = [a, cos, sin, *w]
    specs = [pl.BlockSpec((tile, depth), lambda i, at_ref: (i, 0)), pl.BlockSpec((tile, HEAD // 2), place), pl.BlockSpec((tile, HEAD // 2), place)]
    specs += [pl.BlockSpec((HEAD, 3 * HEAD), lambda i, at_ref: (0, 0))] * 8
    aliases = {}
    if so_far is not None:
        aliases = {1 + len(given) + n: n for n in range(3)}
        given += so_far
        specs += [pl.BlockSpec(memory_space=pl.ANY)] * 3
    return list(pl.pallas_call(
        _project,
        grid_spec=pltpu.PrefetchScalarGridSpec(num_scalar_prefetch=1, grid=(per,), in_specs=specs, out_specs=[pl.BlockSpec((tile, HEAD), place)] * 3),
        out_shape=[jax.ShapeDtypeStruct((everything, HEAD), jnp.bfloat16)] * 3,
        input_output_aliases=aliases,
        compiler_params=pltpu.CompilerParams(dimension_semantics=("arbitrary",), vmem_limit_bytes=VMEM),
        cost_estimate=pl.CostEstimate(flops=2 * tokens * depth * 3 * HEAD, transcendentals=0, bytes_accessed=tokens * depth * 2 + depth * 3 * HEAD * 2),
        name="project",
    )(at, *given))


def _pairs(plan_ref, q_ref, k_ref, v_ref, *rest, carried):
    if carried:
        top_in, mix_in, _, o_ref, top_s, mix_s = rest
    else:
        o_ref, top_s, mix_s = rest
        top_s, mix_s = top_s.at[0], mix_s.at[0]
    t = pl.program_id(0)
    e = HEAD**-0.5 * LOG2E
    strips, blocks = CHUNK // STRIP, CHUNK // KEYS
    ones = jnp.ones((8, KEYS), jnp.bfloat16)

    @pl.when(plan_ref[2, t] == 1)
    def _():
        top_s[...] = jnp.full(top_s.shape, NEG, jnp.float32)
        mix_s[...] = jnp.zeros(mix_s.shape, jnp.float32)

    if carried:

        @pl.when(plan_ref[2, t] == 2)
        def _():
            top_s[...] = top_in[0]
            mix_s[...] = mix_in[0]

    def block(j, first, diagonal):
        here = pl.ds(j * KEYS, KEYS)
        keys = k_ref[here, :]
        values = jnp.concatenate([v_ref[here, :].T, ones], axis=0)
        mine = [slice(n * STRIP, (n + 1) * STRIP) for n in range(first, strips)]
        scores = [_dot(keys, q_ref[at, :], 1, 1) for at in mine]
        weights, keeps = [], []
        for n, (at, s) in enumerate(zip(mine, scores)):
            if diagonal and n == 0:
                s = jnp.where(lax.broadcasted_iota(jnp.int32, s.shape, 1) >= lax.broadcasted_iota(jnp.int32, s.shape, 0), s, 2 * NEG)
            old = top_s[0:1, at]
            top = jnp.maximum(old, s.max(axis=0, keepdims=True))
            top_s[0:1, at] = top
            weights.append(jnp.exp2((s - top) * e).astype(jnp.bfloat16))
            keeps.append(jnp.exp2((old - top) * e))
        for at, p, keep in zip(mine, weights, keeps):
            mix_s[:, at] = mix_s[:, at] * keep + _dot(values, p, 1, 0)

    own = plan_ref[0, t] == plan_ref[1, t]

    @pl.when(jnp.logical_not(own))
    def _():
        lax.fori_loop(0, blocks, lambda j, _: block(j, 0, False), None)

    @pl.when(own)
    def _():
        for j in range(blocks):
            block(j, j, True)

    @pl.when(plan_ref[3, t] == 1)
    def _():
        for n in range(strips):
            at = slice(n * STRIP, (n + 1) * STRIP)
            o_ref[at, :] = (mix_s[:HEAD, at] * (1 / mix_s[HEAD : HEAD + 1, at])).T.astype(o_ref.dtype)


def pairs(plan, q, k, v, units, before=None):
    tokens = q.shape[0]
    chunks = tokens // CHUNK
    chunk = lambda row: pl.BlockSpec((CHUNK, HEAD), lambda t, plan_ref: (plan_ref[row, t], 0))
    state = [pl.BlockSpec((1, 8, CHUNK), lambda t, plan_ref: (plan_ref[0, t], 0, 0)),
             pl.BlockSpec((1, HEAD + 8, CHUNK), lambda t, plan_ref: (plan_ref[0, t], 0, 0))]
    out = jax.ShapeDtypeStruct((tokens, HEAD), jnp.bfloat16)
    if before is None:
        given, specs, aliases, scratch = [], [], {}, []
        shapes = [out, jax.ShapeDtypeStruct((chunks, 8, CHUNK), jnp.float32), jax.ShapeDtypeStruct((chunks, HEAD + 8, CHUNK), jnp.float32)]
        gives = [chunk(0), *state]
    else:
        given = [before[1], before[2], before[0]]
        specs, aliases = [*state, pl.BlockSpec(memory_space=pl.ANY)], {6: 0}
        scratch = [pltpu.VMEM((8, CHUNK), jnp.float32), pltpu.VMEM((HEAD + 8, CHUNK), jnp.float32)]
        shapes, gives = [out], [chunk(0)]
    return pl.pallas_call(
        functools.partial(_pairs, carried=before is not None),
        grid_spec=pltpu.PrefetchScalarGridSpec(num_scalar_prefetch=1, grid=(plan.shape[1],), in_specs=[chunk(0), chunk(1), chunk(1), *specs],
                                               out_specs=gives, scratch_shapes=scratch),
        out_shape=shapes,
        input_output_aliases=aliases,
        compiler_params=pltpu.CompilerParams(dimension_semantics=("arbitrary",), vmem_limit_bytes=VMEM),
        cost_estimate=pl.CostEstimate(flops=int(units * 4 * CHUNK * CHUNK * HEAD * 1.6), transcendentals=int(units * CHUNK * CHUNK), bytes_accessed=2**24),
        name="pairs",
    )(plan, q, k, v, *given)


def plans(far):
    table = []
    for late in range(4):
        near = [n for n in range(4) if n != late]
        a = [(i, j, int(j == near[0]), int(j == i)) for i in near for j in near if j <= i]
        b = [(late, j, int(j == 0), int(j == late)) for j in range(late + 1)] + [(i, late, 2, 1) for i in range(late + 1, 4)]
        table.append(a + b)
    table = jnp.asarray(table, jnp.int32)
    plan = lax.dynamic_index_in_dim(table, far, 0, keepdims=False).T
    return plan[:, :6], plan[:, 6:]


def _finish(x_ref, *rest):
    o_refs, w_refs, y_ref = rest[:8], rest[8:16], rest[16]
    total = None
    for o_ref, w_ref in zip(o_refs, w_refs):
        part = _dot(o_ref[...], w_ref[...], 1, 0)
        total = part if total is None else total + part
    y_ref[...] = (x_ref[...].astype(jnp.float32) + total).astype(y_ref.dtype)


def finish(x, seen, wo):
    tokens, depth = x.shape
    tile = 256
    row = lambda i: (i, 0)
    return pl.pallas_call(
        _finish,
        grid=(tokens // tile,),
        in_specs=[pl.BlockSpec((tile, depth), row)] + [pl.BlockSpec((tile, HEAD), row)] * 8 + [pl.BlockSpec((HEAD, depth), lambda i: (0, 0))] * 8,
        out_specs=pl.BlockSpec((tile, depth), row),
        out_shape=jax.ShapeDtypeStruct(x.shape, x.dtype),
        compiler_params=pltpu.CompilerParams(dimension_semantics=("arbitrary",), vmem_limit_bytes=VMEM),
        cost_estimate=pl.CostEstimate(flops=2 * tokens * depth * depth, transcendentals=0, bytes_accessed=2 * depth * depth + 6 * tokens * depth),
        name="finish",
    )(x, *seen, *wo)


def solution(mesh):
    def step(x, gain, wq, wk, wv, wo):
        own = x.shape[0]
        me = lax.axis_index("sp")
        a = normed(x, gain)

        def columns(d):
            return jnp.concatenate([lax.dynamic_slice_in_dim(w, d * HEAD, HEAD, axis=1) for w in (wq, wk, wv)], axis=1)

        order = [source(me) for source, _ in RELATIONS]
        w, a = exchanged(columns, me, a)
        states = gathered(a)
        half = HEAD // 2
        angle = jnp.arange(8 * own).astype(jnp.float32)[:, None] * THETA ** (-jnp.arange(half, dtype=jnp.float32) / half)
        cos, sin = jnp.cos(angle), jnp.sin(angle)

        qkv = None
        near, far = plans((me ^ 6) // 2)
        for n in (0, 1, 2, 5, 3, 6):
            qkv = project(order[n], w, order, states[n], cos, sin, qkv)
        part = pairs(near, *qkv, 4.5)
        for n in (4, 7):
            qkv = project(order[n], w, order, states[n], cos, sin, qkv)
        wo, _ = lax.optimization_barrier((wo, states[4]))
        (seen,) = pairs(far, *qkv, 3.5, part)
        seen = seen.reshape(8, own, HEAD)
        (seen,) = exchanged(lambda d: lax.dynamic_index_in_dim(seen, d, 0, keepdims=False), me)
        return finish(x, seen, gathered(wo))

    tokens, whole = P(("dp", "sp"), None), P("sp", None)
    return jax.shard_map(
        step,
        mesh=mesh,
        in_specs=(tokens, P(None), whole, whole, whole, whole),
        out_specs=tokens,
        check_vma=False,
    )
```

```python
import functools

import jax
import jax.numpy as jnp
import numpy as np
from jax import lax
from jax.experimental import pallas as pl
from jax.experimental.pallas import tpu as pltpu
from jax.sharding import PartitionSpec as P

NEG = -1e30
LOG2E = 1.4426950408889634
HEAD = 256
HALF = HEAD // 2
THETA = 10000
VMEM = 60 * 2**20
STRIP = 512
KEYS = 512
OWN = 1024
CHUNK = 2048
DEPTH = 2048
TALL = HEAD + 16
MESH = pl.DeviceIdType.MESH


def _dot(a, b, ca, cb):
    return lax.dot_general(a, b, (((ca,), (cb,)), ((), ())), preferred_element_type=jnp.float32)


def tables():
    rate = float(THETA) ** (-np.arange(HALF) / HALF)
    fine, coarse = np.arange(OWN)[:, None] * rate, OWN * np.arange(8)[:, None] * rate
    return [f(t).astype(np.float32) for t in (fine, coarse) for f in (np.cos, np.sin)]


def _body(x_ref, gain_ref, wq_ref, wk_ref, wv_ref, wo_ref, cos_ref, sin_ref, cos8_ref, sin8_ref,
          piece_ref, seen_ref, out_w_ref,
          a_s, x_s, w_s, wo_s, q_s, k_s, vt_s, top_s, mix_s, o_s,
          local, w_send, w_recv, p_send, p_recv, f_send, f_recv, o_send, o_recv):
    me = lax.axis_index("sp")
    x, y, core = me // 4, (me // 2) % 2, me % 2
    late = 3 - me // 2

    def place(n):
        g, k = n // 2, (core + n) % 2
        along_x = jnp.where(g == 1, 1 - k, jnp.where(g == 2, k, jnp.where(g == 3, 1, 0)))
        along_y = jnp.where(g == 1, k, jnp.where(g == 2, 1 - k, jnp.where(g == 3, 1, 0)))
        return 4 * ((x + along_x) % 2) + 2 * ((y + along_y) % 2) + k

    partner, first, second = place(1), place(2), place(4)

    def to(device):
        return {"sp": device}

    def hop(n, own, all_ref, send, recv):
        source = own if n in (1, 2, 4) else all_ref.at[place(n - 1 if n % 2 else 2)]
        carried = me if n in (1, 2, 4) else place(n - 1 if n % 2 else 2)
        target = partner if n % 2 else (first if n == 2 else second)
        return pltpu.make_async_remote_copy(source, all_ref.at[carried], send.at[n], recv.at[n], device_id=to(target), device_id_type=MESH)

    def landed(n, own, all_ref, send, recv):
        pltpu.make_async_remote_copy(own, all_ref.at[place(n)], send.at[n], recv.at[n], device_id=to(partner), device_id_type=MESH).wait_recv()

    state = functools.partial(hop, own=a_s, all_ref=piece_ref, send=p_send, recv=p_recv)
    state_landed = functools.partial(landed, own=a_s, all_ref=piece_ref, send=p_send, recv=p_recv)
    last = functools.partial(hop, own=wo_ref, all_ref=out_w_ref, send=f_send, recv=f_recv)
    last_landed = functools.partial(landed, own=wo_ref, all_ref=out_w_ref, send=f_send, recv=f_recv)

    get_x = pltpu.make_async_copy(x_ref, x_s, local.at[0])
    get_wo = pltpu.make_async_copy(wo_ref, wo_s, local.at[1])
    get_x.start()
    get_wo.start()

    barrier = pltpu.get_barrier_semaphore()
    for step in range(1, 8):
        pl.semaphore_signal(barrier, inc=1, device_id=to((me + step) % 8), device_id_type=MESH)
    pl.semaphore_wait(barrier, 7)

    weights = (wq_ref, wk_ref, wv_ref)

    def columns(m, device):
        return weights[m].at[:, pl.ds(pl.multiple_of(device * HEAD, HEAD), HEAD)]

    def rows(m, device):
        return w_s.at[pl.ds(pl.multiple_of(device * HEAD, HEAD), HEAD), pl.ds(m * HEAD, HEAD)]

    def weight(n, m):
        k = (core + n) % 2
        g, base = n // 2, core
        flip_x = (1 - base if g == 1 else base if g == 2 else 1) if g else 0
        flip_y = (base if g == 1 else 1 - base if g == 2 else 1) if g else 0
        device = 4 * ((x + flip_x) % 2) + 2 * ((y + flip_y) % 2) + k
        return pltpu.make_async_remote_copy(columns(m, device), rows(m, me), w_send.at[3 * n + m], w_recv.at[3 * n + m], device_id=to(device),
                                            device_id_type=MESH)

    for n in (6, 7, 2, 5, 4, 3, 1):
        for m in range(3):
            weight(n, m).start()
    mine = [pltpu.make_async_copy(columns(m, me), rows(m, me), local.at[2 + m]) for m in range(3)]
    for copy in mine:
        copy.start()

    get_x.wait()

    def norm(i, _):
        at = pl.ds(pl.multiple_of(i * 128, 128), 128)
        wide = x_s[at, :].astype(jnp.float32)
        scale = lax.rsqrt(jnp.mean(wide * wide, -1, keepdims=True) + 1e-6)
        a_s[at, :] = (wide * scale * gain_ref[...].astype(jnp.float32)).astype(jnp.bfloat16)

    lax.fori_loop(0, OWN // 128, norm, None)
    state(2).start()
    state(1).start()

    get_wo.wait()
    put_wo = pltpu.make_async_copy(wo_s, out_w_ref.at[me], local.at[1])
    put_wo.start()
    top_s[...] = jnp.full(top_s.shape, NEG, jnp.float32)

    def clear(i, _):
        mix_s[i] = jnp.zeros(mix_s.shape[1:], jnp.float32)

    lax.fori_loop(0, 4, clear, None)
    vt_s[HEAD:, :] = jnp.ones((TALL - HEAD, vt_s.shape[1]), jnp.bfloat16)
    for copy in mine:
        copy.wait()
    for n in range(1, 8):
        for m in range(3):
            pltpu.make_async_remote_copy(columns(m, me), rows(m, place(n)), w_send.at[3 * n + m], w_recv.at[3 * n + m], device_id=to(partner),
                                         device_id_type=MESH).wait_recv()

    def project(source, piece):
        cos8, sin8 = cos8_ref[pl.ds(piece, 1), :], sin8_ref[pl.ds(piece, 1), :]

        def tile(i, _):
            at = pl.ds(pl.multiple_of(i * 256, 256), 256)
            into = pl.ds(pl.multiple_of(piece * OWN + i * 256, 256), 256)
            total = _dot(source[at, :], w_s[...], 1, 0).astype(jnp.bfloat16)
            fine_cos, fine_sin = cos_ref[at, :], sin_ref[at, :]
            cos, sin = fine_cos * cos8 - fine_sin * sin8, fine_sin * cos8 + fine_cos * sin8
            for ref, column in ((q_s, 0), (k_s, HEAD)):
                one, two = total[:, column : column + HALF].astype(jnp.float32), total[:, column + HALF : column + HEAD].astype(jnp.float32)
                ref[into, :HALF] = (one * cos - two * sin).astype(jnp.bfloat16)
                ref[into, HALF:] = (two * cos + one * sin).astype(jnp.bfloat16)
            vt_s[:HEAD, into] = total[:, 2 * HEAD :].T

        lax.fori_loop(0, OWN // 256, tile, None)

    e = HEAD**-0.5 * LOG2E
    strips, blocks = CHUNK // STRIP, CHUNK // KEYS

    def block(qi, ki, j, from_strip, diagonal):
        here = pl.ds(pl.multiple_of(ki * CHUNK + j * KEYS, KEYS), KEYS)
        keys, values = k_s[here, :], vt_s[:, here]
        mine = [slice(n * STRIP, (n + 1) * STRIP) for n in range(from_strip, strips)]
        scores = [_dot(keys, q_s[pl.ds(pl.multiple_of(qi * CHUNK + at.start, STRIP), STRIP), :], 1, 1) for at in mine]
        weights, keeps = [], []
        for n, (at, s) in enumerate(zip(mine, scores)):
            if diagonal and n == 0:
                s = jnp.where(lax.broadcasted_iota(jnp.int32, s.shape, 1) >= lax.broadcasted_iota(jnp.int32, s.shape, 0), s, 2 * NEG)
            old = top_s[qi, 0:1, at]
            top = jnp.maximum(old, s.max(axis=0, keepdims=True))
            top_s[qi, 0:1, at] = top
            weights.append(jnp.exp2((s - top) * e).astype(jnp.bfloat16))
            keeps.append(jnp.exp2((old - top) * e))
        for at, p, keep in zip(mine, weights, keeps):
            mix_s[qi, :, at] = mix_s[qi, :, at] * keep + _dot(values, p, 1, 0)

    def pair(qi, ki):
        @pl.when(qi != ki)
        def _():
            lax.fori_loop(0, blocks, lambda j, _: block(qi, ki, j, 0, False), None)

        @pl.when(qi == ki)
        def _():
            for j in range(blocks):
                block(qi, ki, j, j, True)

    def result(device):
        rows = o_s.at[pl.ds(pl.multiple_of(device * OWN, OWN), OWN), :]
        return pltpu.make_async_remote_copy(rows, seen_ref.at[me], o_send.at[device], o_recv.at[me], device_id=to(device), device_id_type=MESH)

    def own_result():
        return pltpu.make_async_copy(o_s.at[pl.ds(pl.multiple_of(me * OWN, OWN), OWN), :], seen_ref.at[me], local.at[0])

    def finished(qi):
        for n in range(strips):
            at = slice(n * STRIP, (n + 1) * STRIP)
            o_s[pl.ds(pl.multiple_of(qi * CHUNK + at.start, STRIP), STRIP), :] = (
                mix_s[qi, :HEAD, at] * (1 / mix_s[qi, HEAD : HEAD + 1, at])).T.astype(jnp.bfloat16)
        for k in range(2):

            @pl.when(2 * qi + k != me)
            def _():
                result(2 * qi + k).start()

            @pl.when(2 * qi + k == me)
            def _():
                own_result().start()

    near = [jnp.where(late > n, n, n + 1) for n in range(3)]
    chip = 3 - late

    def chunks(t):
        qi = jnp.where(t == 0, chip, jnp.where(t == 1, (chip + 2) % 4, jnp.where(t == 2, chip + 1 - 2 * (chip % 2), jnp.where(t == 3, near[1], near[2]))))
        ki = jnp.where(t < 3, qi, jnp.where(t == 5, near[1], near[0]))
        m = t - 7
        far_q = jnp.where(t == 6, late, jnp.where(m < late, late, m + 1))
        far_k = jnp.where(t == 6, late, jnp.where(m < late, m, late))
        return jnp.where(t < 6, qi, far_q), jnp.where(t < 6, ki, far_k)

    def stage(n, _):
        @pl.when(n == 1)
        def _():
            state_landed(1)

        @pl.when(n == 2)
        def _():
            state_landed(2)
            state(4).start()
            state(6).start()
            state(3).start()

        @pl.when(n == 3)
        def _():
            state_landed(3)

        @pl.when(n == 4)
        def _():
            state_landed(4)
            state(5).start()

        @pl.when(n == 5)
        def _():
            state_landed(5)

        @pl.when(n == 7)
        def _():
            state_landed(7)

        piece = place(n)

        @pl.when(n > 0)
        def _():
            copy = pltpu.make_async_copy(piece_ref.at[piece], x_s, local.at[5])
            copy.start()
            copy.wait()
            project(x_s, piece)

        @pl.when(n == 0)
        def _():
            project(a_s, piece)

        def step(t, _):
            @pl.when(t == 5)
            def _():
                state_landed(6)
                state(7).start()
                last(2).start()
                last(4).start()
                last(1).start()

            @pl.when(t == 6)
            def _():
                last_landed(2)
                last(6).start()
                last(3).start()

            @pl.when(t == 8)
            def _():
                last_landed(4)
                last(5).start()

            @pl.when(t == 9)
            def _():
                last_landed(6)
                last(7).start()

            qi, ki = chunks(t)
            pair(qi, ki)
            done = jnp.where(t < 6, 0, jnp.where(t == 6, jnp.where(late == 0, 1, 0), jnp.where(t - 7 >= late - 1, 1, 0)))

            @pl.when(done == 1)
            def _():
                finished(qi)

            @pl.when(t == 5)
            def _():
                lax.fori_loop(0, late, lambda j, _: finished(j), None)

        start = jnp.where(n == 5, 1, jnp.where(n == 7, 6, 0))
        stop = jnp.where(n == 3, 1, jnp.where(n == 5, 6, jnp.where(n == 7, 10, 0)))
        lax.fori_loop(start, stop, step, None)

    lax.fori_loop(0, 8, stage, None)

    put_wo.wait()
    for n in (1, 3, 5, 7):
        last_landed(n)
    for n in range(1, 8):
        state(n).wait_send()
        last(n).wait_send()
        for m in range(3):
            weight(n, m).wait_send()
    own_result().wait()
    for step in range(1, 8):
        device = (me + step) % 8
        result(device).wait_send()
        pltpu.make_async_remote_copy(o_s.at[pl.ds(0, OWN), :], seen_ref.at[device], o_send.at[device], o_recv.at[device], device_id=to(device),
                                     device_id_type=MESH).wait_recv()


def attended(x, gain, wq, wk, wv, wo):
    hbm, vmem = pl.BlockSpec(memory_space=pl.ANY), pl.BlockSpec(memory_space=pltpu.VMEM)
    dma = pltpu.SemaphoreType.DMA
    low = jnp.bfloat16
    return pl.pallas_call(
        _body,
        in_specs=[hbm, vmem, hbm, hbm, hbm, hbm, vmem, vmem, vmem, vmem],
        out_specs=[hbm] * 3,
        out_shape=[jax.ShapeDtypeStruct((8, OWN, DEPTH), low), jax.ShapeDtypeStruct((8, OWN, HEAD), low), jax.ShapeDtypeStruct((8, HEAD, DEPTH), low)],
        scratch_shapes=[pltpu.VMEM((OWN, DEPTH), low), pltpu.VMEM((OWN, DEPTH), low), pltpu.VMEM((DEPTH, 3 * HEAD), low), pltpu.VMEM((HEAD, DEPTH), low),
                        pltpu.VMEM((8 * OWN, HEAD), low), pltpu.VMEM((8 * OWN, HEAD), low), pltpu.VMEM((TALL, 8 * OWN), low),
                        pltpu.VMEM((4, 8, CHUNK), jnp.float32), pltpu.VMEM((4, TALL, CHUNK), jnp.float32), pltpu.VMEM((8 * OWN, HEAD), low),
                        dma((6,)), dma((24,)), dma((24,)), dma((8,)), dma((8,)), dma((8,)), dma((8,)), dma((8,)), dma((8,))],
        compiler_params=pltpu.CompilerParams(collective_id=0, has_side_effects=True, vmem_limit_bytes=VMEM),
        cost_estimate=pl.CostEstimate(flops=2**36, transcendentals=2**25, bytes_accessed=2**27),
        name="attended",
    )(x, gain, wq, wk, wv, wo, *(jnp.asarray(t) for t in tables()))


def _finish(x_ref, seen_ref, wo_ref, y_ref):
    seen = jnp.concatenate([seen_ref[n] for n in range(8)], axis=1)
    y_ref[...] = (x_ref[...].astype(jnp.float32) + _dot(seen, wo_ref[...], 1, 0)).astype(y_ref.dtype)


def finish(x, seen, wo):
    tokens, depth = x.shape
    tile = 256
    row = lambda i: (i, 0)
    return pl.pallas_call(
        _finish,
        grid=(tokens // tile,),
        in_specs=[pl.BlockSpec((tile, depth), row), pl.BlockSpec((8, tile, HEAD), lambda i: (0, i, 0)), pl.BlockSpec((depth, depth), lambda i: (0, 0))],
        out_specs=pl.BlockSpec((tile, depth), row),
        out_shape=jax.ShapeDtypeStruct(x.shape, x.dtype),
        compiler_params=pltpu.CompilerParams(dimension_semantics=("arbitrary",), vmem_limit_bytes=VMEM),
        cost_estimate=pl.CostEstimate(flops=2 * tokens * depth * depth, transcendentals=0, bytes_accessed=2 * depth * depth + 6 * tokens * depth),
        name="finish",
    )(x, seen, wo)


def solution(mesh):
    def step(x, gain, wq, wk, wv, wo):
        _, seen, whole_wo = attended(x, gain[None], wq, wk, wv, wo)
        return finish(x, seen, whole_wo.reshape(DEPTH, DEPTH))

    tokens, whole = P(("dp", "sp"), None), P("sp", None)
    return jax.shard_map(
        step,
        mesh=mesh,
        in_specs=(tokens, P(None), whole, whole, whole, whole),
        out_specs=tokens,
        check_vma=False,
    )
```

```python
import functools

import jax
import jax.numpy as jnp
import numpy as np
from jax import lax
from jax.experimental import pallas as pl
from jax.experimental.pallas import tpu as pltpu
from jax.sharding import PartitionSpec as P

NEG = -1e30
LOG2E = 1.4426950408889634
HEAD = 256
HALF = HEAD // 2
THETA = 10000
VMEM = 60 * 2**20
STRIP = 512
KEYS = 512
OWN = 1024
CHUNK = 2048
DEPTH = 2048
TALL = HEAD + 16
MESH = pl.DeviceIdType.MESH


def _dot(a, b, ca, cb):
    return lax.dot_general(a, b, (((ca,), (cb,)), ((), ())), preferred_element_type=jnp.float32)


def tables():
    rate = float(THETA) ** (-np.arange(HALF) / HALF)
    fine, coarse = np.arange(OWN)[:, None] * rate, OWN * np.arange(8)[:, None] * rate
    return [f(t).astype(np.float32) for t in (fine, coarse) for f in (np.cos, np.sin)]


def _body(x_ref, gain_ref, wq_ref, wk_ref, wv_ref, wo_ref, cos_ref, sin_ref, cos8_ref, sin8_ref,
          piece_ref, y_ref,
          a_s, x_s, w_s, wo_s, seen_s, q_s, k_s, vt_s, top_s, mix_s, o_s,
          local, w_send, w_recv, p_send, p_recv, f_send, f_recv, o_send, o_recv):
    me = lax.axis_index("sp")
    x, y, core = me // 4, (me // 2) % 2, me % 2
    late = 3 - me // 2

    def place(n):
        g, k = n // 2, (core + n) % 2
        along_x = jnp.where(g == 1, 1 - k, jnp.where(g == 2, k, jnp.where(g == 3, 1, 0)))
        along_y = jnp.where(g == 1, k, jnp.where(g == 2, 1 - k, jnp.where(g == 3, 1, 0)))
        return 4 * ((x + along_x) % 2) + 2 * ((y + along_y) % 2) + k

    partner, first, second = place(1), place(2), place(4)

    def to(device):
        return {"sp": device}

    def hop(n, own, all_ref, send, recv):
        source = own if n in (1, 2, 4) else all_ref.at[place(n - 1 if n % 2 else 2)]
        carried = me if n in (1, 2, 4) else place(n - 1 if n % 2 else 2)
        target = partner if n % 2 else (first if n == 2 else second)
        return pltpu.make_async_remote_copy(source, all_ref.at[carried], send.at[n], recv.at[n], device_id=to(target), device_id_type=MESH)

    def landed(n, own, all_ref, send, recv):
        pltpu.make_async_remote_copy(own, all_ref.at[place(n)], send.at[n], recv.at[n], device_id=to(partner), device_id_type=MESH).wait_recv()

    state = functools.partial(hop, own=a_s, all_ref=piece_ref, send=p_send, recv=p_recv)
    state_landed = functools.partial(landed, own=a_s, all_ref=piece_ref, send=p_send, recv=p_recv)
    last = functools.partial(hop, own=wo_ref, all_ref=wo_s, send=f_send, recv=f_recv)
    last_landed = functools.partial(landed, own=wo_ref, all_ref=wo_s, send=f_send, recv=f_recv)

    get_x = pltpu.make_async_copy(x_ref, x_s, local.at[0])
    get_wo = pltpu.make_async_copy(wo_ref, wo_s.at[me], local.at[1])
    get_x.start()
    get_wo.start()

    barrier = pltpu.get_barrier_semaphore()
    for step in range(1, 8):
        pl.semaphore_signal(barrier, inc=1, device_id=to((me + step) % 8), device_id_type=MESH)
    pl.semaphore_wait(barrier, 7)

    weights = (wq_ref, wk_ref, wv_ref)

    def columns(m, device):
        return weights[m].at[:, pl.ds(pl.multiple_of(device * HEAD, HEAD), HEAD)]

    def rows(m, device):
        return w_s.at[pl.ds(pl.multiple_of(device * HEAD, HEAD), HEAD), pl.ds(m * HEAD, HEAD)]

    def weight(n, m):
        k = (core + n) % 2
        g, base = n // 2, core
        flip_x = (1 - base if g == 1 else base if g == 2 else 1) if g else 0
        flip_y = (base if g == 1 else 1 - base if g == 2 else 1) if g else 0
        device = 4 * ((x + flip_x) % 2) + 2 * ((y + flip_y) % 2) + k
        return pltpu.make_async_remote_copy(columns(m, device), rows(m, me), w_send.at[3 * n + m], w_recv.at[3 * n + m], device_id=to(device),
                                            device_id_type=MESH)

    for n in (6, 7, 2, 5, 4, 3, 1):
        for m in range(3):
            weight(n, m).start()
    mine = [pltpu.make_async_copy(columns(m, me), rows(m, me), local.at[2 + m]) for m in range(3)]
    for copy in mine:
        copy.start()

    get_x.wait()

    def norm(i, _):
        at = pl.ds(pl.multiple_of(i * 128, 128), 128)
        wide = x_s[at, :].astype(jnp.float32)
        scale = lax.rsqrt(jnp.mean(wide * wide, -1, keepdims=True) + 1e-6)
        a_s[at, :] = (wide * scale * gain_ref[...].astype(jnp.float32)).astype(jnp.bfloat16)

    lax.fori_loop(0, OWN // 128, norm, None)
    state(2).start()
    state(1).start()

    top_s[...] = jnp.full(top_s.shape, NEG, jnp.float32)

    def clear(i, _):
        mix_s[i] = jnp.zeros(mix_s.shape[1:], jnp.float32)

    lax.fori_loop(0, 4, clear, None)
    vt_s[HEAD:, :] = jnp.ones((TALL - HEAD, vt_s.shape[1]), jnp.bfloat16)
    for copy in mine:
        copy.wait()
    for n in range(1, 8):
        for m in range(3):
            pltpu.make_async_remote_copy(columns(m, me), rows(m, place(n)), w_send.at[3 * n + m], w_recv.at[3 * n + m], device_id=to(partner),
                                         device_id_type=MESH).wait_recv()

    def project(source, piece):
        cos8, sin8 = cos8_ref[pl.ds(piece, 1), :], sin8_ref[pl.ds(piece, 1), :]

        def tile(i, _):
            at = pl.ds(pl.multiple_of(i * 256, 256), 256)
            into = pl.ds(pl.multiple_of(piece * OWN + i * 256, 256), 256)
            total = _dot(source[at, :], w_s[...], 1, 0).astype(jnp.bfloat16)
            fine_cos, fine_sin = cos_ref[at, :], sin_ref[at, :]
            cos, sin = fine_cos * cos8 - fine_sin * sin8, fine_sin * cos8 + fine_cos * sin8
            for ref, column in ((q_s, 0), (k_s, HEAD)):
                one, two = total[:, column : column + HALF].astype(jnp.float32), total[:, column + HALF : column + HEAD].astype(jnp.float32)
                ref[into, :HALF] = (one * cos - two * sin).astype(jnp.bfloat16)
                ref[into, HALF:] = (two * cos + one * sin).astype(jnp.bfloat16)
            vt_s[:HEAD, into] = total[:, 2 * HEAD :].T

        lax.fori_loop(0, OWN // 256, tile, None)

    e = HEAD**-0.5 * LOG2E
    strips, blocks = CHUNK // STRIP, CHUNK // KEYS

    def block(qi, ki, j, from_strip, diagonal):
        here = pl.ds(pl.multiple_of(ki * CHUNK + j * KEYS, KEYS), KEYS)
        keys, values = k_s[here, :], vt_s[:, here]
        mine = [slice(n * STRIP, (n + 1) * STRIP) for n in range(from_strip, strips)]
        scores = [_dot(keys, q_s[pl.ds(pl.multiple_of(qi * CHUNK + at.start, STRIP), STRIP), :], 1, 1) for at in mine]
        weights, keeps = [], []
        for n, (at, s) in enumerate(zip(mine, scores)):
            if diagonal and n == 0:
                s = jnp.where(lax.broadcasted_iota(jnp.int32, s.shape, 1) >= lax.broadcasted_iota(jnp.int32, s.shape, 0), s, 2 * NEG)
            old = top_s[qi, 0:1, at]
            top = jnp.maximum(old, s.max(axis=0, keepdims=True))
            top_s[qi, 0:1, at] = top
            weights.append(jnp.exp2((s - top) * e).astype(jnp.bfloat16))
            keeps.append(jnp.exp2((old - top) * e))
        for at, p, keep in zip(mine, weights, keeps):
            mix_s[qi, :, at] = mix_s[qi, :, at] * keep + _dot(values, p, 1, 0)

    def pair(qi, ki):
        @pl.when(qi != ki)
        def _():
            lax.fori_loop(0, blocks, lambda j, _: block(qi, ki, j, 0, False), None)

        @pl.when(qi == ki)
        def _():
            for j in range(blocks):
                block(qi, ki, j, j, True)

    def result(device):
        rows = o_s.at[pl.ds(pl.multiple_of(device * OWN, OWN), OWN), :]
        return pltpu.make_async_remote_copy(rows, seen_s.at[me], o_send.at[device], o_recv.at[me], device_id=to(device), device_id_type=MESH)

    def own_result():
        return pltpu.make_async_copy(o_s.at[pl.ds(pl.multiple_of(me * OWN, OWN), OWN), :], seen_s.at[me], local.at[0])

    def finished(qi):
        for n in range(strips):
            at = slice(n * STRIP, (n + 1) * STRIP)
            o_s[pl.ds(pl.multiple_of(qi * CHUNK + at.start, STRIP), STRIP), :] = (
                mix_s[qi, :HEAD, at] * (1 / mix_s[qi, HEAD : HEAD + 1, at])).T.astype(jnp.bfloat16)
        for k in range(2):

            @pl.when(2 * qi + k != me)
            def _():
                result(2 * qi + k).start()

            @pl.when(2 * qi + k == me)
            def _():
                own_result().start()

    near = [jnp.where(late > n, n, n + 1) for n in range(3)]
    chip = 3 - late

    def chunks(t):
        qi = jnp.where(t == 0, chip, jnp.where(t == 1, (chip + 2) % 4, jnp.where(t == 2, chip + 1 - 2 * (chip % 2), jnp.where(t == 3, near[1], near[2]))))
        ki = jnp.where(t < 3, qi, jnp.where(t == 5, near[1], near[0]))
        m = t - 7
        far_q = jnp.where(t == 6, late, jnp.where(m < late, late, m + 1))
        far_k = jnp.where(t == 6, late, jnp.where(m < late, m, late))
        return jnp.where(t < 6, qi, far_q), jnp.where(t < 6, ki, far_k)

    def stage(n, _):
        @pl.when(n == 1)
        def _():
            state_landed(1)

        @pl.when(n == 2)
        def _():
            state_landed(2)
            state(4).start()
            state(6).start()
            state(3).start()

        @pl.when(n == 3)
        def _():
            state_landed(3)

        @pl.when(n == 4)
        def _():
            state_landed(4)
            state(5).start()

        @pl.when(n == 5)
        def _():
            state_landed(5)

        @pl.when(n == 7)
        def _():
            state_landed(7)

        piece = place(n)

        @pl.when(n > 0)
        def _():
            copy = pltpu.make_async_copy(piece_ref.at[piece], x_s, local.at[5])
            copy.start()
            copy.wait()
            project(x_s, piece)

        @pl.when(n == 0)
        def _():
            project(a_s, piece)

        def step(t, _):
            @pl.when(t == 5)
            def _():
                state_landed(6)
                state(7).start()
                last(2).start()
                last(4).start()
                last(1).start()

            @pl.when(t == 7)
            def _():
                last_landed(2)
                last(6).start()
                last(3).start()

            qi, ki = chunks(t)
            pair(qi, ki)
            done = jnp.where(t < 6, 0, jnp.where(t == 6, jnp.where(late == 0, 1, 0), jnp.where(t - 7 >= late - 1, 1, 0)))

            @pl.when(done == 1)
            def _():
                finished(qi)

            @pl.when(t == 5)
            def _():
                lax.fori_loop(0, late, lambda j, _: finished(j), None)

        start = jnp.where(n == 5, 1, jnp.where(n == 7, 6, 0))
        stop = jnp.where(n == 3, 1, jnp.where(n == 5, 6, jnp.where(n == 7, 10, 0)))
        lax.fori_loop(start, stop, step, None)

    lax.fori_loop(0, 8, stage, None)

    get_x = pltpu.make_async_copy(x_ref, x_s, local.at[2])
    get_x.start()
    get_wo.wait()
    own_result().wait()
    last_landed(4)
    last(5).start()
    last_landed(6)
    last(7).start()

    def result_landed(n):
        device = place(n)
        pltpu.make_async_remote_copy(o_s.at[pl.ds(0, OWN), :], seen_s.at[device], o_send.at[device], o_recv.at[device], device_id=to(partner),
                                     device_id_type=MESH).wait_recv()

    def term(n, i):
        device = place(n)
        return _dot(seen_s[device, i * 256 : (i + 1) * 256, :], wo_s[device], 1, 0)

    for i in range(4):
        mix_s[i, :256, :] = term(0, i)
    for n in range(1, 6):
        if n % 2:
            last_landed(n)
        result_landed(n)
        for i in range(4):
            mix_s[i, :256, :] += term(n, i)
    get_x.wait()
    for n in (1, 2, 4):
        state(n).wait_send()
    last_landed(7)
    result_landed(6)
    result_landed(7)
    out = []
    for i in range(4):
        at = slice(i * 256, (i + 1) * 256)
        a_s[at, :] = (x_s[at, :].astype(jnp.float32) + (mix_s[i, :256, :] + term(6, i) + term(7, i))).astype(jnp.bfloat16)
        out += [pltpu.make_async_copy(a_s.at[at, :], y_ref.at[at, :], local.at[2 + i])]
        out[i].start()

    for n in range(1, 8):
        if n not in (1, 2, 4):
            state(n).wait_send()
        last(n).wait_send()
        for m in range(3):
            weight(n, m).wait_send()
    for step in range(1, 8):
        result((me + step) % 8).wait_send()
    for copy in out:
        copy.wait()


def attended(x, gain, wq, wk, wv, wo):
    hbm, vmem = pl.BlockSpec(memory_space=pl.ANY), pl.BlockSpec(memory_space=pltpu.VMEM)
    dma = pltpu.SemaphoreType.DMA
    low = jnp.bfloat16
    return pl.pallas_call(
        _body,
        in_specs=[hbm, vmem, hbm, hbm, hbm, hbm, vmem, vmem, vmem, vmem],
        out_specs=[hbm] * 2,
        out_shape=[jax.ShapeDtypeStruct((8, OWN, DEPTH), low), jax.ShapeDtypeStruct((OWN, DEPTH), low)],
        scratch_shapes=[pltpu.VMEM((OWN, DEPTH), low), pltpu.VMEM((OWN, DEPTH), low), pltpu.VMEM((DEPTH, 3 * HEAD), low), pltpu.VMEM((8, HEAD, DEPTH), low),
                        pltpu.VMEM((8, OWN, HEAD), low),
                        pltpu.VMEM((8 * OWN, HEAD), low), pltpu.VMEM((8 * OWN, HEAD), low), pltpu.VMEM((TALL, 8 * OWN), low),
                        pltpu.VMEM((4, 8, CHUNK), jnp.float32), pltpu.VMEM((4, TALL, CHUNK), jnp.float32), pltpu.VMEM((8 * OWN, HEAD), low),
                        dma((6,)), dma((24,)), dma((24,)), dma((8,)), dma((8,)), dma((8,)), dma((8,)), dma((8,)), dma((8,))],
        compiler_params=pltpu.CompilerParams(collective_id=0, has_side_effects=True, vmem_limit_bytes=VMEM),
        cost_estimate=pl.CostEstimate(flops=2**36, transcendentals=2**25, bytes_accessed=2**27),
        name="attended",
    )(x, gain, wq, wk, wv, wo, *(jnp.asarray(t) for t in tables()))


def solution(mesh):
    def step(x, gain, wq, wk, wv, wo):
        return attended(x, gain, wq, wk, wv, wo)[1]

    tokens, whole = P(("dp", "sp"), None), P("sp", None)
    return jax.shard_map(
        step,
        mesh=mesh,
        in_specs=(tokens, P(None), whole, whole, whole, whole),
        out_specs=tokens,
        check_vma=False,
    )
```

```python
import functools

import jax
import jax.numpy as jnp
import numpy as np
from jax import lax
from jax.experimental import pallas as pl
from jax.experimental.pallas import tpu as pltpu
from jax.sharding import PartitionSpec as P

NEG = -1e30
LOG2E = 1.4426950408889634
HEAD = 256
HALF = HEAD // 2
THETA = 10000
VMEM = 60 * 2**20
STRIP = 512
KEYS = 512
OWN = 1024
CHUNK = 2048
DEPTH = 2048
TALL = HEAD + 16
MESH = pl.DeviceIdType.MESH


def _dot(a, b, ca, cb):
    return lax.dot_general(a, b, (((ca,), (cb,)), ((), ())), preferred_element_type=jnp.float32)


def tables():
    rate = float(THETA) ** (-np.arange(HALF) / HALF)
    fine, coarse = np.arange(OWN)[:, None] * rate, OWN * np.arange(8)[:, None] * rate
    return [f(t).astype(np.float32) for t in (fine, coarse) for f in (np.cos, np.sin)]


def _body(x_ref, gain_ref, wq_ref, wk_ref, wv_ref, wo_ref, cos_ref, sin_ref, cos8_ref, sin8_ref,
          piece_ref, y_ref,
          a_s, x_s, w_s, wo_s, seen_s, q_s, k_s, vt_s, top_s, mix_s, o_s,
          local, w_send, w_recv, p_send, p_recv, f_send, f_recv, o_send, o_recv):
    me = lax.axis_index("sp")
    x, y, core = me // 4, (me // 2) % 2, me % 2
    late = 3 - me // 2

    def place(n):
        g, k = n // 2, (core + n) % 2
        along_x = jnp.where(g == 1, 1 - k, jnp.where(g == 2, k, jnp.where(g == 3, 1, 0)))
        along_y = jnp.where(g == 1, k, jnp.where(g == 2, 1 - k, jnp.where(g == 3, 1, 0)))
        return 4 * ((x + along_x) % 2) + 2 * ((y + along_y) % 2) + k

    partner, first, second = place(1), place(2), place(4)

    def to(device):
        return {"sp": device}

    def hop(n, own, all_ref, send, recv):
        source = own if n in (1, 2, 4) else all_ref.at[place(n - 1 if n % 2 else 2)]
        carried = me if n in (1, 2, 4) else place(n - 1 if n % 2 else 2)
        target = partner if n % 2 else (first if n == 2 else second)
        return pltpu.make_async_remote_copy(source, all_ref.at[carried], send.at[n], recv.at[n], device_id=to(target), device_id_type=MESH)

    def landed(n, own, all_ref, send, recv):
        pltpu.make_async_remote_copy(own, all_ref.at[place(n)], send.at[n], recv.at[n], device_id=to(partner), device_id_type=MESH).wait_recv()

    state = functools.partial(hop, own=a_s, all_ref=piece_ref, send=p_send, recv=p_recv)
    state_landed = functools.partial(landed, own=a_s, all_ref=piece_ref, send=p_send, recv=p_recv)
    last = functools.partial(hop, own=wo_ref, all_ref=wo_s, send=f_send, recv=f_recv)
    last_landed = functools.partial(landed, own=wo_ref, all_ref=wo_s, send=f_send, recv=f_recv)

    get_x = pltpu.make_async_copy(x_ref, x_s, local.at[0])
    get_wo = pltpu.make_async_copy(wo_ref, wo_s.at[me], local.at[1])
    get_x.start()
    get_wo.start()

    barrier = pltpu.get_barrier_semaphore()
    for step in range(1, 8):
        pl.semaphore_signal(barrier, inc=1, device_id=to((me + step) % 8), device_id_type=MESH)
    pl.semaphore_wait(barrier, 7)

    weights = (wq_ref, wk_ref, wv_ref)

    def columns(m, device):
        return weights[m].at[:, pl.ds(pl.multiple_of(device * HEAD, HEAD), HEAD)]

    def rows(m, device):
        return w_s.at[pl.ds(pl.multiple_of(device * HEAD, HEAD), HEAD), pl.ds(m * HEAD, HEAD)]

    def weight(n, m):
        k = (core + n) % 2
        g, base = n // 2, core
        flip_x = (1 - base if g == 1 else base if g == 2 else 1) if g else 0
        flip_y = (base if g == 1 else 1 - base if g == 2 else 1) if g else 0
        device = 4 * ((x + flip_x) % 2) + 2 * ((y + flip_y) % 2) + k
        return pltpu.make_async_remote_copy(columns(m, device), rows(m, me), w_send.at[3 * n + m], w_recv.at[3 * n + m], device_id=to(device),
                                            device_id_type=MESH)

    for n in (6, 7, 2, 5, 4, 3, 1):
        for m in range(3):
            weight(n, m).start()
    mine = [pltpu.make_async_copy(columns(m, me), rows(m, me), local.at[2 + m]) for m in range(3)]
    for copy in mine:
        copy.start()

    get_x.wait()

    def norm(i, _):
        at = pl.ds(pl.multiple_of(i * 128, 128), 128)
        wide = x_s[at, :].astype(jnp.float32)
        scale = lax.rsqrt(jnp.mean(wide * wide, -1, keepdims=True) + 1e-6)
        a_s[at, :] = (wide * scale * gain_ref[...].astype(jnp.float32)).astype(jnp.bfloat16)

    lax.fori_loop(0, OWN // 128, norm, None)
    state(2).start()
    state(1).start()

    top_s[...] = jnp.full(top_s.shape, NEG, jnp.float32)

    def clear(i, _):
        mix_s[i] = jnp.zeros(mix_s.shape[1:], jnp.float32)

    lax.fori_loop(0, 4, clear, None)
    vt_s[HEAD:, :] = jnp.ones((TALL - HEAD, vt_s.shape[1]), jnp.bfloat16)
    for copy in mine:
        copy.wait()
    for n in range(1, 8):
        for m in range(3):
            pltpu.make_async_remote_copy(columns(m, me), rows(m, place(n)), w_send.at[3 * n + m], w_recv.at[3 * n + m], device_id=to(partner),
                                         device_id_type=MESH).wait_recv()

    def project(source, piece):
        cos8, sin8 = cos8_ref[pl.ds(piece, 1), :], sin8_ref[pl.ds(piece, 1), :]

        def tile(i, _):
            at = pl.ds(pl.multiple_of(i * 256, 256), 256)
            into = pl.ds(pl.multiple_of(piece * OWN + i * 256, 256), 256)
            total = _dot(source[at, :], w_s[...], 1, 0).astype(jnp.bfloat16)
            fine_cos, fine_sin = cos_ref[at, :], sin_ref[at, :]
            cos, sin = fine_cos * cos8 - fine_sin * sin8, fine_sin * cos8 + fine_cos * sin8
            for ref, column in ((q_s, 0), (k_s, HEAD)):
                one, two = total[:, column : column + HALF].astype(jnp.float32), total[:, column + HALF : column + HEAD].astype(jnp.float32)
                ref[into, :HALF] = (one * cos - two * sin).astype(jnp.bfloat16)
                ref[into, HALF:] = (two * cos + one * sin).astype(jnp.bfloat16)
            vt_s[:HEAD, into] = total[:, 2 * HEAD :].T

        lax.fori_loop(0, OWN // 256, tile, None)

    e = HEAD**-0.5 * LOG2E
    strips, blocks = CHUNK // STRIP, CHUNK // KEYS

    def block(qi, ki, j, from_strip, diagonal):
        here = pl.ds(pl.multiple_of(ki * CHUNK + j * KEYS, KEYS), KEYS)
        keys, values = k_s[here, :], vt_s[:, here]
        mine = [slice(n * STRIP, (n + 1) * STRIP) for n in range(from_strip, strips)]
        scores = [_dot(keys, q_s[pl.ds(pl.multiple_of(qi * CHUNK + at.start, STRIP), STRIP), :], 1, 1) for at in mine]
        weights, keeps = [], []
        for n, (at, s) in enumerate(zip(mine, scores)):
            if diagonal and n == 0:
                s = jnp.where(lax.broadcasted_iota(jnp.int32, s.shape, 1) >= lax.broadcasted_iota(jnp.int32, s.shape, 0), s, 2 * NEG)
            old = top_s[qi, 0:1, at]
            top = jnp.maximum(old, s.max(axis=0, keepdims=True))
            top_s[qi, 0:1, at] = top
            weights.append(jnp.exp2((s - top) * e).astype(jnp.bfloat16))
            keeps.append(jnp.exp2((old - top) * e))
        for at, p, keep in zip(mine, weights, keeps):
            mix_s[qi, :, at] = mix_s[qi, :, at] * keep + _dot(values, p, 1, 0)

    def pair(qi, ki):
        @pl.when(qi != ki)
        def _():
            lax.fori_loop(0, blocks, lambda j, _: block(qi, ki, j, 0, False), None)

        @pl.when(qi == ki)
        def _():
            for j in range(blocks):
                block(qi, ki, j, j, True)

    def result(device):
        rows = o_s.at[pl.ds(pl.multiple_of(device * OWN, OWN), OWN), :]
        return pltpu.make_async_remote_copy(rows, seen_s.at[me], o_send.at[device], o_recv.at[me], device_id=to(device), device_id_type=MESH)

    def own_result():
        return pltpu.make_async_copy(o_s.at[pl.ds(pl.multiple_of(me * OWN, OWN), OWN), :], seen_s.at[me], local.at[0])

    def finished(qi):
        for n in range(strips):
            at = slice(n * STRIP, (n + 1) * STRIP)
            o_s[pl.ds(pl.multiple_of(qi * CHUNK + at.start, STRIP), STRIP), :] = (
                mix_s[qi, :HEAD, at] * (1 / mix_s[qi, HEAD : HEAD + 1, at])).T.astype(jnp.bfloat16)
        for k in range(2):

            @pl.when(2 * qi + k != me)
            def _():
                result(2 * qi + k).start()

            @pl.when(2 * qi + k == me)
            def _():
                own_result().start()

    near = [jnp.where(late > n, n, n + 1) for n in range(3)]
    chip = 3 - late

    table = (((1, 0, 1), (2, 0, 1), (0, 0, 1), (3, 0, 1)), ((3, 1, 1), (1, 1, 0), (1, 0, 1), (2, 1, 1)),
             ((3, 2, 1), (2, 2, 0), (2, 0, 0), (2, 1, 1)), ((3, 3, 0), (3, 0, 0), (3, 1, 0), (3, 2, 1)))

    def far(t):
        def pick(values, index):
            return jnp.where(index == 0, values[0], jnp.where(index == 1, values[1], jnp.where(index == 2, values[2], values[3])))

        return [pick([pick([entry[part] for entry in row], t - 6) for row in table], late) for part in range(3)]

    def chunks(t):
        qi = jnp.where(t == 0, chip, jnp.where(t == 1, (chip + 2) % 4, jnp.where(t == 2, chip + 1 - 2 * (chip % 2), jnp.where(t == 3, near[1], near[2]))))
        ki = jnp.where(t < 3, qi, jnp.where(t == 5, near[1], near[0]))
        far_q, far_k, _ = far(t)
        return jnp.where(t < 6, qi, far_q), jnp.where(t < 6, ki, far_k)

    def stage(n, _):
        @pl.when(n == 1)
        def _():
            state_landed(1)

        @pl.when(n == 2)
        def _():
            state_landed(2)
            state(4).start()
            state(6).start()
            state(3).start()
            last(4).start()

        @pl.when(n == 3)
        def _():
            state_landed(3)

        @pl.when(n == 4)
        def _():
            state_landed(4)
            state(5).start()

        @pl.when(n == 5)
        def _():
            state_landed(5)

        @pl.when(n == 7)
        def _():
            state_landed(7)

        piece = place(n)

        @pl.when(n > 0)
        def _():
            copy = pltpu.make_async_copy(piece_ref.at[piece], x_s, local.at[5])
            copy.start()
            copy.wait()
            project(x_s, piece)

        @pl.when(n == 0)
        def _():
            project(a_s, piece)

        def step(t, _):
            @pl.when(t == 5)
            def _():
                state_landed(6)
                state(7).start()
                last(2).start()
                last(1).start()

            @pl.when(t == 8)
            def _():
                last_landed(4)
                last(5).start()

            qi, ki = chunks(t)
            pair(qi, ki)

            @pl.when(t == 6)
            def _():
                last_landed(2)
                last(6).start()
                last(3).start()
                lax.fori_loop(0, late, lambda j, _: finished(j), None)

            @pl.when((t > 5) & (far(t)[2] == 1))
            def _():
                finished(qi)

        start = jnp.where(n == 5, 1, jnp.where(n == 7, 6, 0))
        stop = jnp.where(n == 3, 1, jnp.where(n == 5, 6, jnp.where(n == 7, 10, 0)))
        lax.fori_loop(start, stop, step, None)

    lax.fori_loop(0, 8, stage, None)

    get_x = pltpu.make_async_copy(x_ref, x_s, local.at[2])
    get_x.start()
    get_wo.wait()
    own_result().wait()
    last_landed(6)
    last(7).start()

    def result_landed(n):
        device = place(n)
        pltpu.make_async_remote_copy(o_s.at[pl.ds(0, OWN), :], seen_s.at[device], o_send.at[device], o_recv.at[device], device_id=to(partner),
                                     device_id_type=MESH).wait_recv()

    def term(n, i):
        device = place(n)
        return _dot(seen_s[device, i * 256 : (i + 1) * 256, :], wo_s[device], 1, 0)

    for i in range(4):
        mix_s[i, :256, :] = term(0, i)
    for n in range(1, 6):
        if n % 2:
            last_landed(n)
        result_landed(n)
        for i in range(4):
            mix_s[i, :256, :] += term(n, i)
    get_x.wait()
    for n in (1, 2, 4):
        state(n).wait_send()
    last_landed(7)
    result_landed(6)
    result_landed(7)
    out = []
    for i in range(4):
        at = slice(i * 256, (i + 1) * 256)
        a_s[at, :] = (x_s[at, :].astype(jnp.float32) + (mix_s[i, :256, :] + term(6, i) + term(7, i))).astype(jnp.bfloat16)
        out += [pltpu.make_async_copy(a_s.at[at, :], y_ref.at[at, :], local.at[2 + i])]
        out[i].start()

    for n in range(1, 8):
        if n not in (1, 2, 4):
            state(n).wait_send()
        last(n).wait_send()
        for m in range(3):
            weight(n, m).wait_send()
    for step in range(1, 8):
        result((me + step) % 8).wait_send()
    for copy in out:
        copy.wait()


def attended(x, gain, wq, wk, wv, wo):
    hbm, vmem = pl.BlockSpec(memory_space=pl.ANY), pl.BlockSpec(memory_space=pltpu.VMEM)
    dma = pltpu.SemaphoreType.DMA
    low = jnp.bfloat16
    return pl.pallas_call(
        _body,
        in_specs=[hbm, vmem, hbm, hbm, hbm, hbm, vmem, vmem, vmem, vmem],
        out_specs=[hbm] * 2,
        out_shape=[jax.ShapeDtypeStruct((8, OWN, DEPTH), low), jax.ShapeDtypeStruct((OWN, DEPTH), low)],
        scratch_shapes=[pltpu.VMEM((OWN, DEPTH), low), pltpu.VMEM((OWN, DEPTH), low), pltpu.VMEM((DEPTH, 3 * HEAD), low), pltpu.VMEM((8, HEAD, DEPTH), low),
                        pltpu.VMEM((8, OWN, HEAD), low),
                        pltpu.VMEM((8 * OWN, HEAD), low), pltpu.VMEM((8 * OWN, HEAD), low), pltpu.VMEM((TALL, 8 * OWN), low),
                        pltpu.VMEM((4, 8, CHUNK), jnp.float32), pltpu.VMEM((4, TALL, CHUNK), jnp.float32), pltpu.VMEM((8 * OWN, HEAD), low),
                        dma((6,)), dma((24,)), dma((24,)), dma((8,)), dma((8,)), dma((8,)), dma((8,)), dma((8,)), dma((8,))],
        compiler_params=pltpu.CompilerParams(collective_id=0, has_side_effects=True, vmem_limit_bytes=VMEM),
        cost_estimate=pl.CostEstimate(flops=2**36, transcendentals=2**25, bytes_accessed=2**27),
        name="attended",
    )(x, gain, wq, wk, wv, wo, *(jnp.asarray(t) for t in tables()))


def solution(mesh):
    def step(x, gain, wq, wk, wv, wo):
        return attended(x, gain, wq, wk, wv, wo)[1]

    tokens, whole = P(("dp", "sp"), None), P("sp", None)
    return jax.shard_map(
        step,
        mesh=mesh,
        in_specs=(tokens, P(None), whole, whole, whole, whole),
        out_specs=tokens,
        check_vma=False,
    )
```

```python
import functools

import jax
import jax.numpy as jnp
import numpy as np
from jax import lax
from jax.experimental import pallas as pl
from jax.experimental.pallas import tpu as pltpu
from jax.sharding import PartitionSpec as P

NEG = -1e30
LOG2E = 1.4426950408889634
HEAD = 256
HALF = HEAD // 2
THETA = 10000
VMEM = 58 * 2**20
STRIP = 512
KEYS = 512
OWN = 1024
CUT = 768
CHUNK = 2048
DEPTH = 2048
TALL = HEAD + 16
MESH = pl.DeviceIdType.MESH


def _dot(a, b, ca, cb):
    return lax.dot_general(a, b, (((ca,), (cb,)), ((), ())), preferred_element_type=jnp.float32)


def tables():
    rate = float(THETA) ** (-np.arange(HALF) / HALF)
    fine, coarse = np.arange(OWN)[:, None] * rate, OWN * np.arange(8)[:, None] * rate
    return [f(t).astype(np.float32) for t in (fine, coarse) for f in (np.cos, np.sin)]


def _body(x_ref, gain_ref, wq_ref, wk_ref, wv_ref, wo_ref, cos_in, sin_in, cos8_ref, sin8_ref,
          piece_ref, y_ref,
          cos_ref, sin_ref, a_s, x_s, w_s, wo_s, seen_s, q_s, k_s, vt_s, top_s, mix_s, o_s,
          local, w_send, w_recv, p_send, p_recv, f_send, f_recv, o_send, o_recv):
    me = lax.axis_index("sp")
    x, y, core = me // 4, (me // 2) % 2, me % 2
    late = 3 - me // 2

    def place(n):
        g, k = n // 2, (core + n) % 2
        along_x = jnp.where(g == 1, 1 - k, jnp.where(g == 2, k, jnp.where(g == 3, 1, 0)))
        along_y = jnp.where(g == 1, k, jnp.where(g == 2, 1 - k, jnp.where(g == 3, 1, 0)))
        return 4 * ((x + along_x) % 2) + 2 * ((y + along_y) % 2) + k

    partner, first, second = place(1), place(2), place(4)

    def to(device):
        return {"sp": device}

    def part(ref, n, all_ref):
        if all_ref is not piece_ref or n not in (2, 8):
            return ref
        return ref.at[pl.ds(0, CUT)] if n == 2 else ref.at[pl.ds(CUT, OWN - CUT)]

    def hop(n, own, all_ref, send, recv):
        first_hand = n in (1, 2, 4, 8)
        carried = me if first_hand else place(n - 1 if n % 2 else 2)
        source = own if first_hand else all_ref.at[carried]
        target = partner if n % 2 else (first if n in (2, 8) else second)
        return pltpu.make_async_remote_copy(part(source, n, all_ref), part(all_ref.at[carried], n, all_ref), send.at[n], recv.at[n],
                                            device_id=to(target), device_id_type=MESH)

    def landed(n, own, all_ref, send, recv):
        pltpu.make_async_remote_copy(part(own, n, all_ref), part(all_ref.at[place(2 if n == 8 else n)], n, all_ref), send.at[n], recv.at[n],
                                     device_id=to(partner), device_id_type=MESH).wait_recv()

    state = functools.partial(hop, own=a_s, all_ref=piece_ref, send=p_send, recv=p_recv)
    state_landed = functools.partial(landed, own=a_s, all_ref=piece_ref, send=p_send, recv=p_recv)
    last = functools.partial(hop, own=wo_ref, all_ref=wo_s, send=f_send, recv=f_recv)
    last_landed = functools.partial(landed, own=wo_ref, all_ref=wo_s, send=f_send, recv=f_recv)

    get_x = pltpu.make_async_copy(x_ref, x_s, local.at[0])
    get_wo = pltpu.make_async_copy(wo_ref, wo_s.at[me], local.at[1])
    get_tables = [pltpu.make_async_copy(cos_in, cos_ref, local.at[6]), pltpu.make_async_copy(sin_in, sin_ref, local.at[7])]
    get_x.start()

    barrier = pltpu.get_barrier_semaphore()
    for step in range(1, 8):
        pl.semaphore_signal(barrier, inc=1, device_id=to((me + step) % 8), device_id_type=MESH)
    pl.semaphore_wait(barrier, 7)

    weights = (wq_ref, wk_ref, wv_ref)

    def columns(m, device):
        return weights[m].at[:, pl.ds(pl.multiple_of(device * HEAD, HEAD), HEAD)]

    def rows(m, device):
        return w_s.at[pl.ds(pl.multiple_of(device * HEAD, HEAD), HEAD), pl.ds(m * HEAD, HEAD)]

    def weight(n, m):
        k = (core + n) % 2
        g, base = n // 2, core
        flip_x = (1 - base if g == 1 else base if g == 2 else 1) if g else 0
        flip_y = (base if g == 1 else 1 - base if g == 2 else 1) if g else 0
        device = 4 * ((x + flip_x) % 2) + 2 * ((y + flip_y) % 2) + k
        return pltpu.make_async_remote_copy(columns(m, device), rows(m, me), w_send.at[3 * n + m], w_recv.at[3 * n + m], device_id=to(device),
                                            device_id_type=MESH)

    for n in (6, 7, 2, 5, 4, 3, 1):
        for m in range(3):
            weight(n, m).start()
    mine = [pltpu.make_async_copy(columns(m, me), rows(m, me), local.at[2 + m]) for m in range(3)]
    for copy in mine:
        copy.start()

    for copy in (get_wo, *get_tables):
        copy.start()
    get_x.wait()

    def norm(i, _):
        at = pl.ds(pl.multiple_of(i * 128, 128), 128)
        wide = x_s[at, :].astype(jnp.float32)
        scale = lax.rsqrt(jnp.mean(wide * wide, -1, keepdims=True) + 1e-6)
        a_s[at, :] = (wide * scale * gain_ref[...].astype(jnp.float32)).astype(jnp.bfloat16)

    lax.fori_loop(0, OWN // 128, norm, None)
    state(2).start()
    state(8).start()
    state(1).start()

    top_s[...] = jnp.full(top_s.shape, NEG, jnp.float32)

    def clear(i, _):
        mix_s[i] = jnp.zeros(mix_s.shape[1:], jnp.float32)

    lax.fori_loop(0, 4, clear, None)
    vt_s[HEAD:, :] = jnp.ones((TALL - HEAD, vt_s.shape[1]), jnp.bfloat16)
    for copy in (*mine, *get_tables):
        copy.wait()
    for n in range(1, 8):
        for m in range(3):
            pltpu.make_async_remote_copy(columns(m, me), rows(m, place(n)), w_send.at[3 * n + m], w_recv.at[3 * n + m], device_id=to(partner),
                                         device_id_type=MESH).wait_recv()

    def project(source, piece):
        cos8, sin8 = cos8_ref[pl.ds(piece, 1), :], sin8_ref[pl.ds(piece, 1), :]

        def tile(i, _):
            at = pl.ds(pl.multiple_of(i * 256, 256), 256)
            into = pl.ds(pl.multiple_of(piece * OWN + i * 256, 256), 256)
            total = _dot(source[at, :], w_s[...], 1, 0).astype(jnp.bfloat16)
            fine_cos, fine_sin = cos_ref[at, :], sin_ref[at, :]
            cos, sin = fine_cos * cos8 - fine_sin * sin8, fine_sin * cos8 + fine_cos * sin8
            for ref, column in ((q_s, 0), (k_s, HEAD)):
                one, two = total[:, column : column + HALF].astype(jnp.float32), total[:, column + HALF : column + HEAD].astype(jnp.float32)
                ref[into, :HALF] = (one * cos - two * sin).astype(jnp.bfloat16)
                ref[into, HALF:] = (two * cos + one * sin).astype(jnp.bfloat16)
            vt_s[:HEAD, into] = total[:, 2 * HEAD :].T

        lax.fori_loop(0, OWN // 256, tile, None)

    e = HEAD**-0.5 * LOG2E
    strips, blocks = CHUNK // STRIP, CHUNK // KEYS

    def block(qi, ki, j, from_strip, diagonal):
        here = pl.ds(pl.multiple_of(ki * CHUNK + j * KEYS, KEYS), KEYS)
        keys, values = k_s[here, :], vt_s[:, here]
        mine = [slice(n * STRIP, (n + 1) * STRIP) for n in range(from_strip, strips)]
        scores = [_dot(keys, q_s[pl.ds(pl.multiple_of(qi * CHUNK + at.start, STRIP), STRIP), :], 1, 1) for at in mine]
        weights, keeps = [], []
        for n, (at, s) in enumerate(zip(mine, scores)):
            if diagonal and n == 0:
                s = jnp.where(lax.broadcasted_iota(jnp.int32, s.shape, 1) >= lax.broadcasted_iota(jnp.int32, s.shape, 0), s, 2 * NEG)
            old = top_s[qi, 0:1, at]
            top = jnp.maximum(old, s.max(axis=0, keepdims=True))
            top_s[qi, 0:1, at] = top
            weights.append(jnp.exp2((s - top) * e).astype(jnp.bfloat16))
            keeps.append(jnp.exp2((old - top) * e))
        for at, p, keep in zip(mine, weights, keeps):
            mix_s[qi, :, at] = mix_s[qi, :, at] * keep + _dot(values, p, 1, 0)

    def pair(qi, ki):
        @pl.when(qi != ki)
        def _():
            lax.fori_loop(0, blocks, lambda j, _: block(qi, ki, j, 0, False), None)

        @pl.when(qi == ki)
        def _():
            for j in range(blocks):
                block(qi, ki, j, j, True)

    def result(device):
        rows = o_s.at[pl.ds(pl.multiple_of(device * OWN, OWN), OWN), :]
        return pltpu.make_async_remote_copy(rows, seen_s.at[me], o_send.at[device], o_recv.at[me], device_id=to(device), device_id_type=MESH)

    def own_result():
        return pltpu.make_async_copy(o_s.at[pl.ds(pl.multiple_of(me * OWN, OWN), OWN), :], seen_s.at[me], local.at[0])

    def finished(qi):
        for n in range(strips):
            at = slice(n * STRIP, (n + 1) * STRIP)
            o_s[pl.ds(pl.multiple_of(qi * CHUNK + at.start, STRIP), STRIP), :] = (
                mix_s[qi, :HEAD, at] * (1 / mix_s[qi, HEAD : HEAD + 1, at])).T.astype(jnp.bfloat16)
        for k in range(2):

            @pl.when(2 * qi + k != me)
            def _():
                result(2 * qi + k).start()

            @pl.when(2 * qi + k == me)
            def _():
                own_result().start()

    near = [jnp.where(late > n, n, n + 1) for n in range(3)]
    chip = 3 - late

    table = (((1, 0, 1), (2, 0, 1), (0, 0, 1), (3, 0, 1)), ((3, 1, 1), (1, 1, 0), (1, 0, 1), (2, 1, 1)),
             ((3, 2, 1), (2, 2, 0), (2, 0, 0), (2, 1, 1)), ((3, 3, 0), (3, 0, 0), (3, 1, 0), (3, 2, 1)))

    def far(t):
        def pick(values, index):
            return jnp.where(index == 0, values[0], jnp.where(index == 1, values[1], jnp.where(index == 2, values[2], values[3])))

        return [pick([pick([entry[part] for entry in row], t - 6) for row in table], late) for part in range(3)]

    def chunks(t):
        qi = jnp.where(t == 0, chip, jnp.where(t == 1, (chip + 2) % 4, jnp.where(t == 2, chip + 1 - 2 * (chip % 2), jnp.where(t == 3, near[1], near[2]))))
        ki = jnp.where(t < 3, qi, jnp.where(t == 5, near[1], near[0]))
        far_q, far_k, _ = far(t)
        return jnp.where(t < 6, qi, far_q), jnp.where(t < 6, ki, far_k)

    def stage(n, _):
        @pl.when(n == 1)
        def _():
            state_landed(1)

        @pl.when(n == 2)
        def _():
            state_landed(2)
            state(4).start()
            state_landed(8)
            state(6).start()
            state(3).start()
            last(4).start()

        @pl.when(n == 3)
        def _():
            state_landed(3)

        @pl.when(n == 4)
        def _():
            state_landed(4)
            state(5).start()

        @pl.when(n == 5)
        def _():
            state_landed(5)

        @pl.when(n == 7)
        def _():
            state_landed(7)

        piece = place(n)

        @pl.when(n > 0)
        def _():
            copy = pltpu.make_async_copy(piece_ref.at[piece], x_s, local.at[5])
            copy.start()
            copy.wait()
            project(x_s, piece)

        @pl.when(n == 0)
        def _():
            project(a_s, piece)

        def step(t, _):
            @pl.when(t == 5)
            def _():
                state_landed(6)
                state(7).start()
                last(2).start()
                last(1).start()

            @pl.when(t == 8)
            def _():
                last_landed(4)
                last(5).start()

            qi, ki = chunks(t)
            pair(qi, ki)

            @pl.when(t == 6)
            def _():
                last_landed(2)
                last(6).start()
                last(3).start()

            @pl.when(t == 5)
            def _():
                lax.fori_loop(0, late, lambda j, _: finished(j), None)

            @pl.when((t > 5) & (far(t)[2] == 1))
            def _():
                finished(qi)

        start = jnp.where(n == 5, 1, jnp.where(n == 7, 6, 0))
        stop = jnp.where(n == 3, 1, jnp.where(n == 5, 6, jnp.where(n == 7, 10, 0)))
        lax.fori_loop(start, stop, step, None)

    lax.fori_loop(0, 8, stage, None)

    get_x = pltpu.make_async_copy(x_ref, x_s, local.at[2])
    get_x.start()
    get_wo.wait()
    own_result().wait()

    def result_landed(n):
        device = place(n)
        pltpu.make_async_remote_copy(o_s.at[pl.ds(0, OWN), :], seen_s.at[device], o_send.at[device], o_recv.at[device], device_id=to(partner),
                                     device_id_type=MESH).wait_recv()

    def term(n, i):
        device = place(n)
        return _dot(seen_s[device, i * 256 : (i + 1) * 256, :], wo_s[device], 1, 0)

    for i in range(4):
        mix_s[i, :256, :] = term(0, i)
    get_x.wait()
    for n in range(1, 8):
        if n == 4:
            last_landed(6)
            last(7).start()
        if n % 2:
            last_landed(n)
        result_landed(n)
        if n < 7:
            for i in range(4):
                mix_s[i, :256, :] += term(n, i)
    for i in range(4):
        at = slice(i * 256, (i + 1) * 256)
        y_ref[at, :] = (x_s[at, :].astype(jnp.float32) + (mix_s[i, :256, :] + term(7, i))).astype(jnp.bfloat16)

    state(8).wait_send()
    for n in range(1, 8):
        state(n).wait_send()
        last(n).wait_send()
        for m in range(3):
            weight(n, m).wait_send()
    for step in range(1, 8):
        result((me + step) % 8).wait_send()


def attended(x, gain, wq, wk, wv, wo):
    hbm, vmem = pl.BlockSpec(memory_space=pl.ANY), pl.BlockSpec(memory_space=pltpu.VMEM)
    dma = pltpu.SemaphoreType.DMA
    low = jnp.bfloat16
    return pl.pallas_call(
        _body,
        in_specs=[hbm, vmem, hbm, hbm, hbm, hbm, hbm, hbm, vmem, vmem],
        out_specs=[hbm, vmem],
        out_shape=[jax.ShapeDtypeStruct((8, OWN, DEPTH), low), pltpu.VMEM((OWN, DEPTH), low)],
        scratch_shapes=[pltpu.VMEM((OWN, HALF), jnp.float32), pltpu.VMEM((OWN, HALF), jnp.float32),
                        pltpu.VMEM((OWN, DEPTH), low), pltpu.VMEM((OWN, DEPTH), low), pltpu.VMEM((DEPTH, 3 * HEAD), low), pltpu.VMEM((8, HEAD, DEPTH), low),
                        pltpu.VMEM((8, OWN, HEAD), low),
                        pltpu.VMEM((8 * OWN, HEAD), low), pltpu.VMEM((8 * OWN, HEAD), low), pltpu.VMEM((TALL, 8 * OWN), low),
                        pltpu.VMEM((4, 8, CHUNK), jnp.float32), pltpu.VMEM((4, TALL, CHUNK), jnp.float32), pltpu.VMEM((8 * OWN, HEAD), low),
                        dma((8,)), dma((24,)), dma((24,)), dma((9,)), dma((9,)), dma((8,)), dma((8,)), dma((8,)), dma((8,))],
        compiler_params=pltpu.CompilerParams(collective_id=0, has_side_effects=True, vmem_limit_bytes=VMEM),
        cost_estimate=pl.CostEstimate(flops=2**36, transcendentals=2**25, bytes_accessed=2**27),
        name="attended",
    )(x, gain, wq, wk, wv, wo, *(jnp.asarray(t) for t in tables()))


def solution(mesh):
    def step(x, gain, wq, wk, wv, wo):
        return attended(x, gain, wq, wk, wv, wo)[1]

    tokens, whole = P(("dp", "sp"), None), P("sp", None)
    return jax.shard_map(
        step,
        mesh=mesh,
        in_specs=(tokens, P(None), whole, whole, whole, whole),
        out_specs=tokens,
        check_vma=False,
    )
```

```python
import functools

import jax
import jax.numpy as jnp
import numpy as np
from jax import lax
from jax.experimental import pallas as pl
from jax.experimental.pallas import tpu as pltpu
from jax.sharding import PartitionSpec as P

NEG = -1e30
LOG2E = 1.4426950408889634
HEAD = 256
HALF = HEAD // 2
THETA = 10000
VMEM = 58 * 2**20
STRIP = 512
KEYS = 512
OWN = 1024
CUT = 768
CHUNK = 2048
DEPTH = 2048
TALL = HEAD + 16
MESH = pl.DeviceIdType.MESH


def _dot(a, b, ca, cb):
    return lax.dot_general(a, b, (((ca,), (cb,)), ((), ())), preferred_element_type=jnp.float32)


def tables():
    rate = float(THETA) ** (-np.arange(HALF) / HALF)
    fine, coarse = np.arange(OWN)[:, None] * rate, OWN * np.arange(8)[:, None] * rate
    return [f(t).astype(np.float32) for t in (fine, coarse) for f in (np.cos, np.sin)]


def _body(x_ref, gain_ref, wq_ref, wk_ref, wv_ref, wo_ref, cos_in, sin_in, cos8_ref, sin8_ref,
          piece_ref, y_ref,
          cos_ref, sin_ref, a_s, x_s, w_s, wo_s, seen_s, q_s, k_s, vt_s, top_s, mix_s, o_s,
          local, w_send, w_recv, p_send, p_recv, f_send, f_recv, o_send, o_recv):
    me = lax.axis_index("sp")
    x, y, core = me // 4, (me // 2) % 2, me % 2
    chip = me // 2
    late = 3 - chip

    def place(n):
        g, k = n // 2, (core + n) % 2
        along_x = jnp.where(g == 1, 1 - k, jnp.where(g == 2, k, jnp.where(g == 3, 1, 0)))
        along_y = jnp.where(g == 1, k, jnp.where(g == 2, 1 - k, jnp.where(g == 3, 1, 0)))
        return 4 * ((x + along_x) % 2) + 2 * ((y + along_y) % 2) + k

    partner, first, second = place(1), place(2), place(4)

    def to(device):
        return {"sp": device}

    def part(ref, n, all_ref):
        if all_ref is not piece_ref or n not in (2, 8):
            return ref
        return ref.at[pl.ds(0, CUT)] if n == 2 else ref.at[pl.ds(CUT, OWN - CUT)]

    def hop(n, own, all_ref, send, recv):
        first_hand = n in (1, 2, 4, 8)
        carried = me if first_hand else place(n - 1 if n % 2 else 2)
        source = own if first_hand else all_ref.at[carried]
        target = partner if n % 2 else (first if n in (2, 8) else second)
        return pltpu.make_async_remote_copy(part(source, n, all_ref), part(all_ref.at[carried], n, all_ref), send.at[n], recv.at[n],
                                            device_id=to(target), device_id_type=MESH)

    def landed(n, own, all_ref, send, recv):
        pltpu.make_async_remote_copy(part(own, n, all_ref), part(all_ref.at[place(2 if n == 8 else n)], n, all_ref), send.at[n], recv.at[n],
                                     device_id=to(partner), device_id_type=MESH).wait_recv()

    state = functools.partial(hop, own=a_s, all_ref=piece_ref, send=p_send, recv=p_recv)
    state_landed = functools.partial(landed, own=a_s, all_ref=piece_ref, send=p_send, recv=p_recv)
    last = functools.partial(hop, own=wo_ref, all_ref=wo_s, send=f_send, recv=f_recv)
    last_landed = functools.partial(landed, own=wo_ref, all_ref=wo_s, send=f_send, recv=f_recv)

    get_x = pltpu.make_async_copy(x_ref, x_s, local.at[0])
    get_wo = pltpu.make_async_copy(wo_ref, wo_s.at[me], local.at[1])
    get_tables = [pltpu.make_async_copy(cos_in, cos_ref, local.at[6]), pltpu.make_async_copy(sin_in, sin_ref, local.at[7])]
    get_x.start()

    barrier = pltpu.get_barrier_semaphore()
    for step in range(1, 8):
        pl.semaphore_signal(barrier, inc=1, device_id=to((me + step) % 8), device_id_type=MESH)
    pl.semaphore_wait(barrier, 7)

    weights = (wq_ref, wk_ref, wv_ref)

    def columns(m, device):
        return weights[m].at[:, pl.ds(pl.multiple_of(device * HEAD, HEAD), HEAD)]

    def rows(m, device):
        return w_s.at[pl.ds(pl.multiple_of(device * HEAD, HEAD), HEAD), pl.ds(m * HEAD, HEAD)]

    def weight(n, m):
        k = (core + n) % 2
        g, base = n // 2, core
        flip_x = (1 - base if g == 1 else base if g == 2 else 1) if g else 0
        flip_y = (base if g == 1 else 1 - base if g == 2 else 1) if g else 0
        device = 4 * ((x + flip_x) % 2) + 2 * ((y + flip_y) % 2) + k
        return pltpu.make_async_remote_copy(columns(m, device), rows(m, me), w_send.at[3 * n + m], w_recv.at[3 * n + m], device_id=to(device),
                                            device_id_type=MESH)

    for n in (6, 7, 2, 5, 4, 3, 1):
        for m in range(3):
            weight(n, m).start()
    mine = [pltpu.make_async_copy(columns(m, me), rows(m, me), local.at[2 + m]) for m in range(3)]
    for copy in mine:
        copy.start()

    for copy in (get_wo, *get_tables):
        copy.start()
    get_x.wait()

    def norm(i, _):
        at = pl.ds(pl.multiple_of(i * 128, 128), 128)
        wide = x_s[at, :].astype(jnp.float32)
        scale = lax.rsqrt(jnp.mean(wide * wide, -1, keepdims=True) + 1e-6)
        a_s[at, :] = (wide * scale * gain_ref[...].astype(jnp.float32)).astype(jnp.bfloat16)

    lax.fori_loop(0, OWN // 128, norm, None)
    state(2).start()
    state(8).start()
    state(1).start()

    top_s[...] = jnp.full(top_s.shape, NEG, jnp.float32)

    def clear(i, _):
        mix_s[i] = jnp.zeros(mix_s.shape[1:], jnp.float32)

    lax.fori_loop(0, 4, clear, None)
    vt_s[HEAD:, :] = jnp.ones((TALL - HEAD, vt_s.shape[1]), jnp.bfloat16)
    for copy in (*mine, *get_tables):
        copy.wait()
    for n in range(1, 8):
        for m in range(3):
            pltpu.make_async_remote_copy(columns(m, me), rows(m, place(n)), w_send.at[3 * n + m], w_recv.at[3 * n + m], device_id=to(partner),
                                         device_id_type=MESH).wait_recv()

    def project(source, piece):
        cos8, sin8 = cos8_ref[pl.ds(piece, 1), :], sin8_ref[pl.ds(piece, 1), :]

        def tile(i, _):
            at = pl.ds(pl.multiple_of(i * 256, 256), 256)
            into = pl.ds(pl.multiple_of(piece * OWN + i * 256, 256), 256)
            total = _dot(source[at, :], w_s[...], 1, 0).astype(jnp.bfloat16)
            fine_cos, fine_sin = cos_ref[at, :], sin_ref[at, :]
            cos, sin = fine_cos * cos8 - fine_sin * sin8, fine_sin * cos8 + fine_cos * sin8
            for ref, column in ((q_s, 0), (k_s, HEAD)):
                one, two = total[:, column : column + HALF].astype(jnp.float32), total[:, column + HALF : column + HEAD].astype(jnp.float32)
                ref[into, :HALF] = (one * cos - two * sin).astype(jnp.bfloat16)
                ref[into, HALF:] = (two * cos + one * sin).astype(jnp.bfloat16)
            vt_s[:HEAD, into] = total[:, 2 * HEAD :].T

        lax.fori_loop(0, OWN // 256, tile, None)

    e = HEAD**-0.5 * LOG2E
    strips, blocks = CHUNK // STRIP, CHUNK // KEYS

    def block(qi, ki, j, from_strip, diagonal):
        here = pl.ds(pl.multiple_of(ki * CHUNK + j * KEYS, KEYS), KEYS)
        keys, values = k_s[here, :], vt_s[:, here]
        mine = [slice(n * STRIP, (n + 1) * STRIP) for n in range(from_strip, strips)]
        scores = [_dot(keys, q_s[pl.ds(pl.multiple_of(qi * CHUNK + at.start, STRIP), STRIP), :], 1, 1) for at in mine]
        weights, keeps = [], []
        for n, (at, s) in enumerate(zip(mine, scores)):
            if diagonal and n == 0:
                s = jnp.where(lax.broadcasted_iota(jnp.int32, s.shape, 1) >= lax.broadcasted_iota(jnp.int32, s.shape, 0), s, 2 * NEG)
            old = top_s[qi, 0:1, at]
            top = jnp.maximum(old, s.max(axis=0, keepdims=True))
            top_s[qi, 0:1, at] = top
            weights.append(jnp.exp2((s - top) * e).astype(jnp.bfloat16))
            keeps.append(jnp.exp2((old - top) * e))
        for at, p, keep in zip(mine, weights, keeps):
            mix_s[qi, :, at] = mix_s[qi, :, at] * keep + _dot(values, p, 1, 0)

    def pair(qi, ki):
        @pl.when(qi != ki)
        def _():
            lax.fori_loop(0, blocks, lambda j, _: block(qi, ki, j, 0, False), None)

        @pl.when(qi == ki)
        def _():
            for j in range(blocks):
                block(qi, ki, j, j, True)

    def result(device):
        rows = o_s.at[pl.ds(pl.multiple_of(device * OWN, OWN), OWN), :]
        return pltpu.make_async_remote_copy(rows, seen_s.at[me], o_send.at[device], o_recv.at[me], device_id=to(device), device_id_type=MESH)

    def own_result():
        return pltpu.make_async_copy(o_s.at[pl.ds(pl.multiple_of(me * OWN, OWN), OWN), :], seen_s.at[me], local.at[0])

    def finished(qi):
        for n in range(strips):
            at = slice(n * STRIP, (n + 1) * STRIP)
            o_s[pl.ds(pl.multiple_of(qi * CHUNK + at.start, STRIP), STRIP), :] = (
                mix_s[qi, :HEAD, at] * (1 / mix_s[qi, HEAD : HEAD + 1, at])).T.astype(jnp.bfloat16)

    def keep(qi):
        @pl.when(qi == chip)
        def _():
            own_result().start()
            result(partner).start()

    def early(qi, _):
        finished(qi)
        keep(qi)

        @pl.when(qi != chip)
        def _():
            result(2 * qi + core).start()
            result(2 * qi + 1 - core).start()

    near = [jnp.where(late > n, n, n + 1) for n in range(3)]

    table = (((1, 0, 1), (2, 0, 1), (0, 0, 1), (3, 0, 1)), ((3, 1, 1), (1, 1, 0), (1, 0, 1), (2, 1, 1)),
             ((3, 2, 1), (2, 2, 0), (2, 0, 0), (2, 1, 1)), ((3, 3, 0), (3, 0, 0), (3, 1, 0), (3, 2, 1)))

    def far(t):
        def pick(values, index):
            return jnp.where(index == 0, values[0], jnp.where(index == 1, values[1], jnp.where(index == 2, values[2], values[3])))

        return [pick([pick([entry[part] for entry in row], t - 6) for row in table], late) for part in range(3)]

    def chunks(t):
        qi = jnp.where(t == 0, chip, jnp.where(t == 1, (chip + 2) % 4, jnp.where(t == 2, chip + 1 - 2 * (chip % 2), jnp.where(t == 3, near[1], near[2]))))
        ki = jnp.where(t < 3, qi, jnp.where(t == 5, near[1], near[0]))
        far_q, far_k, _ = far(t)
        return jnp.where(t < 6, qi, far_q), jnp.where(t < 6, ki, far_k)

    def stage(n, _):
        @pl.when(n == 1)
        def _():
            state_landed(1)

        @pl.when(n == 2)
        def _():
            state_landed(2)
            state(4).start()
            state_landed(8)
            state(6).start()
            state(3).start()
            last(4).start()

        @pl.when(n == 3)
        def _():
            state_landed(3)

        @pl.when(n == 4)
        def _():
            state_landed(4)
            state(5).start()

        @pl.when(n == 5)
        def _():
            state_landed(5)

        @pl.when(n == 6)
        def _():
            state_landed(6)
            state(7).start()
            last(2).start()
            last(1).start()
            lax.fori_loop(0, late, early, None)

        @pl.when(n == 7)
        def _():
            state_landed(7)

        piece = place(n)

        @pl.when(n > 0)
        def _():
            copy = pltpu.make_async_copy(piece_ref.at[piece], x_s, local.at[5])
            copy.start()
            copy.wait()
            project(x_s, piece)

        @pl.when(n == 0)
        def _():
            project(a_s, piece)

        def step(t, _):
            @pl.when(t == 8)
            def _():
                last_landed(4)
                last(5).start()

            @pl.when(t == 7)
            def _():
                last_landed(2)
                last(6).start()
                last(3).start()

            qi, ki = chunks(t)
            pair(qi, ki)


            @pl.when((t > 5) & (far(t)[2] == 1))
            def _():
                finished(qi)
                keep(qi)

                @pl.when(qi != chip)
                def _():
                    result(2 * qi + core).start()
                    result(2 * qi + 1 - core).start()

        start = jnp.where(n == 5, 1, jnp.where(n == 7, 6, 0))
        stop = jnp.where(n == 3, 1, jnp.where(n == 5, 6, jnp.where(n == 7, 10, 0)))
        lax.fori_loop(start, stop, step, None)

    lax.fori_loop(0, 8, stage, None)

    get_x = pltpu.make_async_copy(x_ref, x_s, local.at[2])
    get_x.start()
    get_wo.wait()
    own_result().wait()

    def result_landed(n):
        device = place(n)
        pltpu.make_async_remote_copy(o_s.at[pl.ds(0, OWN), :], seen_s.at[device], o_send.at[device], o_recv.at[device], device_id=to(partner),
                                     device_id_type=MESH).wait_recv()

    def term(n, i):
        device = place(n)
        return _dot(seen_s[device, i * 256 : (i + 1) * 256, :], wo_s[device], 1, 0)

    for i in range(4):
        mix_s[i, :256, :] = term(0, i)
    get_x.wait()
    for n in range(1, 8):
        if n == 4:
            last_landed(6)
            last(7).start()
        if n % 2:
            last_landed(n)
        result_landed(n)
        if n < 7:
            for i in range(4):
                mix_s[i, :256, :] += term(n, i)
    for i in range(4):
        at = slice(i * 256, (i + 1) * 256)
        y_ref[at, :] = (x_s[at, :].astype(jnp.float32) + (mix_s[i, :256, :] + term(7, i))).astype(jnp.bfloat16)

    state(8).wait_send()
    for n in range(1, 8):
        state(n).wait_send()
        last(n).wait_send()
        for m in range(3):
            weight(n, m).wait_send()
    for step in range(1, 8):
        result((me + step) % 8).wait_send()


def attended(x, gain, wq, wk, wv, wo):
    hbm, vmem = pl.BlockSpec(memory_space=pl.ANY), pl.BlockSpec(memory_space=pltpu.VMEM)
    dma = pltpu.SemaphoreType.DMA
    low = jnp.bfloat16
    return pl.pallas_call(
        _body,
        in_specs=[hbm, vmem, hbm, hbm, hbm, hbm, hbm, hbm, vmem, vmem],
        out_specs=[hbm, vmem],
        out_shape=[jax.ShapeDtypeStruct((8, OWN, DEPTH), low), pltpu.VMEM((OWN, DEPTH), low)],
        scratch_shapes=[pltpu.VMEM((OWN, HALF), jnp.float32), pltpu.VMEM((OWN, HALF), jnp.float32),
                        pltpu.VMEM((OWN, DEPTH), low), pltpu.VMEM((OWN, DEPTH), low), pltpu.VMEM((DEPTH, 3 * HEAD), low), pltpu.VMEM((8, HEAD, DEPTH), low),
                        pltpu.VMEM((8, OWN, HEAD), low),
                        pltpu.VMEM((8 * OWN, HEAD), low), pltpu.VMEM((8 * OWN, HEAD), low), pltpu.VMEM((TALL, 8 * OWN), low),
                        pltpu.VMEM((4, 8, CHUNK), jnp.float32), pltpu.VMEM((4, TALL, CHUNK), jnp.float32), pltpu.VMEM((8 * OWN, HEAD), low),
                        dma((8,)), dma((24,)), dma((24,)), dma((9,)), dma((9,)), dma((8,)), dma((8,)), dma((8,)), dma((8,))],
        compiler_params=pltpu.CompilerParams(collective_id=0, has_side_effects=True, vmem_limit_bytes=VMEM),
        cost_estimate=pl.CostEstimate(flops=2**36, transcendentals=2**25, bytes_accessed=2**27),
        name="attended",
    )(x, gain, wq, wk, wv, wo, *(jnp.asarray(t) for t in tables()))


def solution(mesh):
    def step(x, gain, wq, wk, wv, wo):
        return attended(x, gain, wq, wk, wv, wo)[1]

    tokens, whole = P(("dp", "sp"), None), P("sp", None)
    return jax.shard_map(
        step,
        mesh=mesh,
        in_specs=(tokens, P(None), whole, whole, whole, whole),
        out_specs=tokens,
        check_vma=False,
    )
```

```python
import functools

import jax
import jax.numpy as jnp
import numpy as np
from jax import lax
from jax.experimental import pallas as pl
from jax.experimental.pallas import tpu as pltpu
from jax.sharding import PartitionSpec as P

NEG = -1e30
LOG2E = 1.4426950408889634
HEAD = 256
HALF = HEAD // 2
THETA = 10000
VMEM = 58 * 2**20
STRIP = 512
KEYS = 512
OWN = 1024
CUT = 768
CHUNK = 2048
DEPTH = 2048
TALL = HEAD + 16
MESH = pl.DeviceIdType.MESH


def _dot(a, b, ca, cb):
    return lax.dot_general(a, b, (((ca,), (cb,)), ((), ())), preferred_element_type=jnp.float32)


def tables():
    rate = float(THETA) ** (-np.arange(HALF) / HALF)
    fine, coarse = np.arange(OWN)[:, None] * rate, OWN * np.arange(8)[:, None] * rate
    return [f(t).astype(np.float32) for t in (fine, coarse) for f in (np.cos, np.sin)]


def _body(x_ref, gain_in, wq_ref, wk_ref, wv_ref, wo_ref, cos_in, sin_in, cos8_in, sin8_in,
          piece_ref, y_ref,
          gain_ref, cos_ref, sin_ref, cos8_ref, sin8_ref, a_s, x_s, w_s, wo_s, seen_s, q_s, k_s, vt_s, top_s, mix_s, o_s,
          local, w_send, w_recv, p_send, p_recv, f_send, f_recv, o_send, o_recv):
    me = lax.axis_index("sp")
    x, y, core = me // 4, (me // 2) % 2, me % 2
    chip = me // 2
    late = 3 - chip

    def place(n):
        g, k = n // 2, (core + n) % 2
        along_x = jnp.where(g == 1, 1 - k, jnp.where(g == 2, k, jnp.where(g == 3, 1, 0)))
        along_y = jnp.where(g == 1, k, jnp.where(g == 2, 1 - k, jnp.where(g == 3, 1, 0)))
        return 4 * ((x + along_x) % 2) + 2 * ((y + along_y) % 2) + k

    partner, first, second = place(1), place(2), place(4)

    def to(device):
        return {"sp": device}

    def part(ref, n, all_ref):
        if all_ref is not piece_ref or n not in (2, 8):
            return ref
        return ref.at[pl.ds(0, CUT)] if n == 2 else ref.at[pl.ds(CUT, OWN - CUT)]

    def hop(n, own, all_ref, send, recv):
        first_hand = n in (1, 2, 4, 8)
        carried = me if first_hand else place(n - 1 if n % 2 else 2)
        source = own if first_hand else all_ref.at[carried]
        target = partner if n % 2 else (first if n in (2, 8) else second)
        return pltpu.make_async_remote_copy(part(source, n, all_ref), part(all_ref.at[carried], n, all_ref), send.at[n], recv.at[n],
                                            device_id=to(target), device_id_type=MESH)

    def landed(n, own, all_ref, send, recv):
        pltpu.make_async_remote_copy(part(own, n, all_ref), part(all_ref.at[place(2 if n == 8 else n)], n, all_ref), send.at[n], recv.at[n],
                                     device_id=to(partner), device_id_type=MESH).wait_recv()

    state = functools.partial(hop, own=a_s, all_ref=piece_ref, send=p_send, recv=p_recv)
    state_landed = functools.partial(landed, own=a_s, all_ref=piece_ref, send=p_send, recv=p_recv)
    last = functools.partial(hop, own=wo_ref, all_ref=wo_s, send=f_send, recv=f_recv)
    last_landed = functools.partial(landed, own=wo_ref, all_ref=wo_s, send=f_send, recv=f_recv)

    get_x = pltpu.make_async_copy(x_ref, x_s, local.at[0])
    get_wo = pltpu.make_async_copy(wo_ref, wo_s.at[me], local.at[1])
    get_tables = [pltpu.make_async_copy(cos_in, cos_ref, local.at[6]), pltpu.make_async_copy(sin_in, sin_ref, local.at[7]),
                  pltpu.make_async_copy(cos8_in, cos8_ref, local.at[8]), pltpu.make_async_copy(sin8_in, sin8_ref, local.at[9])]
    get_gain = pltpu.make_async_copy(gain_in, gain_ref, local.at[10])
    get_x.start()
    get_gain.start()

    barrier = pltpu.get_barrier_semaphore()
    for step in range(1, 8):
        pl.semaphore_signal(barrier, inc=1, device_id=to((me + step) % 8), device_id_type=MESH)
    pl.semaphore_wait(barrier, 7)

    weights = (wq_ref, wk_ref, wv_ref)

    def columns(m, device):
        return weights[m].at[:, pl.ds(pl.multiple_of(device * HEAD, HEAD), HEAD)]

    def rows(m, device):
        return w_s.at[pl.ds(pl.multiple_of(device * HEAD, HEAD), HEAD), pl.ds(m * HEAD, HEAD)]

    def weight(n, m):
        k = (core + n) % 2
        g, base = n // 2, core
        flip_x = (1 - base if g == 1 else base if g == 2 else 1) if g else 0
        flip_y = (base if g == 1 else 1 - base if g == 2 else 1) if g else 0
        device = 4 * ((x + flip_x) % 2) + 2 * ((y + flip_y) % 2) + k
        return pltpu.make_async_remote_copy(columns(m, device), rows(m, me), w_send.at[3 * n + m], w_recv.at[3 * n + m], device_id=to(device),
                                            device_id_type=MESH)

    for n in (6, 7, 2, 5, 4, 3, 1):
        for m in range(3):
            weight(n, m).start()
    mine = [pltpu.make_async_copy(columns(m, me), rows(m, me), local.at[2 + m]) for m in range(3)]
    for copy in mine:
        copy.start()

    for copy in (get_wo, *get_tables):
        copy.start()
    get_x.wait()
    get_gain.wait()

    def norm(i, _):
        at = pl.ds(pl.multiple_of(i * 128, 128), 128)
        wide = x_s[at, :].astype(jnp.float32)
        scale = lax.rsqrt(jnp.mean(wide * wide, -1, keepdims=True) + 1e-6)
        a_s[at, :] = (wide * scale * gain_ref[...].astype(jnp.float32)).astype(jnp.bfloat16)

    lax.fori_loop(0, OWN // 128, norm, None)
    state(2).start()
    state(8).start()
    state(1).start()

    top_s[...] = jnp.full(top_s.shape, NEG, jnp.float32)

    def clear(i, _):
        mix_s[i] = jnp.zeros(mix_s.shape[1:], jnp.float32)

    lax.fori_loop(0, 4, clear, None)
    vt_s[HEAD:, :] = jnp.ones((TALL - HEAD, vt_s.shape[1]), jnp.bfloat16)
    for copy in (*mine, *get_tables):
        copy.wait()
    for n in range(1, 8):
        for m in range(3):
            pltpu.make_async_remote_copy(columns(m, me), rows(m, place(n)), w_send.at[3 * n + m], w_recv.at[3 * n + m], device_id=to(partner),
                                         device_id_type=MESH).wait_recv()

    def project(source, piece):
        cos8, sin8 = cos8_ref[pl.ds(piece, 1), :], sin8_ref[pl.ds(piece, 1), :]

        def tile(i, _):
            at = pl.ds(pl.multiple_of(i * 256, 256), 256)
            into = pl.ds(pl.multiple_of(piece * OWN + i * 256, 256), 256)
            total = _dot(source[at, :], w_s[...], 1, 0).astype(jnp.bfloat16)
            fine_cos, fine_sin = cos_ref[at, :], sin_ref[at, :]
            cos, sin = fine_cos * cos8 - fine_sin * sin8, fine_sin * cos8 + fine_cos * sin8
            for ref, column in ((q_s, 0), (k_s, HEAD)):
                one, two = total[:, column : column + HALF].astype(jnp.float32), total[:, column + HALF : column + HEAD].astype(jnp.float32)
                ref[into, :HALF] = (one * cos - two * sin).astype(jnp.bfloat16)
                ref[into, HALF:] = (two * cos + one * sin).astype(jnp.bfloat16)
            vt_s[:HEAD, into] = total[:, 2 * HEAD :].T

        lax.fori_loop(0, OWN // 256, tile, None)

    e = HEAD**-0.5 * LOG2E
    strips, blocks = CHUNK // STRIP, CHUNK // KEYS

    def block(qi, ki, j, from_strip, diagonal):
        here = pl.ds(pl.multiple_of(ki * CHUNK + j * KEYS, KEYS), KEYS)
        keys, values = k_s[here, :], vt_s[:, here]
        mine = [slice(n * STRIP, (n + 1) * STRIP) for n in range(from_strip, strips)]
        scores = [_dot(keys, q_s[pl.ds(pl.multiple_of(qi * CHUNK + at.start, STRIP), STRIP), :], 1, 1) for at in mine]
        weights, keeps = [], []
        for n, (at, s) in enumerate(zip(mine, scores)):
            if diagonal and n == 0:
                s = jnp.where(lax.broadcasted_iota(jnp.int32, s.shape, 1) >= lax.broadcasted_iota(jnp.int32, s.shape, 0), s, 2 * NEG)
            old = top_s[qi, 0:1, at]
            top = jnp.maximum(old, s.max(axis=0, keepdims=True))
            top_s[qi, 0:1, at] = top
            weights.append(jnp.exp2((s - top) * e).astype(jnp.bfloat16))
            keeps.append(jnp.exp2((old - top) * e))
        for at, p, keep in zip(mine, weights, keeps):
            mix_s[qi, :, at] = mix_s[qi, :, at] * keep + _dot(values, p, 1, 0)

    def pair(qi, ki):
        @pl.when(qi != ki)
        def _():
            lax.fori_loop(0, blocks, lambda j, _: block(qi, ki, j, 0, False), None)

        @pl.when(qi == ki)
        def _():
            for j in range(blocks):
                block(qi, ki, j, j, True)

    def result(device, half):
        rows = o_s.at[pl.ds(pl.multiple_of(device * OWN + half * 512, 512), 512), :]
        return pltpu.make_async_remote_copy(rows, seen_s.at[me, pl.ds(half * 512, 512)], o_send.at[2 * device + half], o_recv.at[2 * me + half],
                                            device_id=to(device), device_id_type=MESH)

    def send(device):
        for half in range(2):
            result(device, half).start()

    def own_result():
        return pltpu.make_async_copy(o_s.at[pl.ds(pl.multiple_of(me * OWN, OWN), OWN), :], seen_s.at[me], local.at[0])

    def finished(qi):
        for n in range(strips):
            at = slice(n * STRIP, (n + 1) * STRIP)
            o_s[pl.ds(pl.multiple_of(qi * CHUNK + at.start, STRIP), STRIP), :] = (
                mix_s[qi, :HEAD, at] * (1 / mix_s[qi, HEAD : HEAD + 1, at])).T.astype(jnp.bfloat16)

    def keep(qi):
        @pl.when(qi == chip)
        def _():
            own_result().start()
            send(partner)

    def early(qi, _):
        finished(qi)
        keep(qi)

        @pl.when(qi != chip)
        def _():
            send(2 * qi + core)
            send(2 * qi + 1 - core)

    near = [jnp.where(late > n, n, n + 1) for n in range(3)]

    table = (((2, 0, 1), (1, 0, 1), (0, 0, 1), (3, 0, 1)), ((3, 1, 1), (1, 1, 0), (1, 0, 1), (2, 1, 1)),
             ((3, 2, 1), (2, 2, 0), (2, 0, 0), (2, 1, 1)), ((3, 3, 0), (3, 0, 0), (3, 1, 0), (3, 2, 1)))

    def far(t):
        def pick(values, index):
            return jnp.where(index == 0, values[0], jnp.where(index == 1, values[1], jnp.where(index == 2, values[2], values[3])))

        return [pick([pick([entry[part] for entry in row], t - 6) for row in table], late) for part in range(3)]

    def chunks(t):
        qi = jnp.where(t == 0, chip, jnp.where(t == 1, (chip + 2) % 4, jnp.where(t == 2, chip + 1 - 2 * (chip % 2), jnp.where(t == 3, near[1], near[2]))))
        ki = jnp.where(t < 3, qi, jnp.where(t == 5, near[1], near[0]))
        far_q, far_k, _ = far(t)
        return jnp.where(t < 6, qi, far_q), jnp.where(t < 6, ki, far_k)

    def stage(n, _):
        @pl.when(n == 1)
        def _():
            state_landed(1)

        @pl.when(n == 2)
        def _():
            state_landed(2)
            state(4).start()
            state_landed(8)
            state(6).start()
            state(3).start()
            last(4).start()

        @pl.when(n == 3)
        def _():
            state_landed(3)

        @pl.when(n == 4)
        def _():
            state_landed(4)
            state(5).start()

        @pl.when(n == 5)
        def _():
            state_landed(5)

        @pl.when(n == 6)
        def _():
            state_landed(6)
            state(7).start()
            last(2).start()
            last(1).start()
            lax.fori_loop(0, late, early, None)

        @pl.when(n == 7)
        def _():
            state_landed(7)

        piece = place(n)

        @pl.when(n > 0)
        def _():
            copy = pltpu.make_async_copy(piece_ref.at[piece], x_s, local.at[5])
            copy.start()
            copy.wait()
            project(x_s, piece)

        @pl.when(n == 0)
        def _():
            project(a_s, piece)

        def step(t, _):
            @pl.when(t == 8)
            def _():
                last_landed(4)
                last(5).start()

            @pl.when(t == 7)
            def _():
                last_landed(2)
                last(6).start()
                last(3).start()

            qi, ki = chunks(t)
            pair(qi, ki)


            @pl.when((t > 5) & (far(t)[2] == 1))
            def _():
                finished(qi)
                keep(qi)

                @pl.when(qi != chip)
                def _():
                    send(2 * qi + core)
                    send(2 * qi + 1 - core)

        start = jnp.where(n == 5, 1, jnp.where(n == 7, 6, 0))
        stop = jnp.where(n == 3, 1, jnp.where(n == 5, 6, jnp.where(n == 7, 10, 0)))
        lax.fori_loop(start, stop, step, None)

    lax.fori_loop(0, 8, stage, None)

    get_x = pltpu.make_async_copy(x_ref, x_s, local.at[2])
    get_x.start()
    get_wo.wait()
    own_result().wait()

    def result_landed(n, half):
        device = place(n)
        pltpu.make_async_remote_copy(o_s.at[pl.ds(0, 512), :], seen_s.at[device, pl.ds(half * 512, 512)], o_send.at[2 * device + half],
                                     o_recv.at[2 * device + half], device_id=to(partner), device_id_type=MESH).wait_recv()

    def term(n, i):
        device = place(n)
        return _dot(seen_s[device, i * 256 : (i + 1) * 256, :], wo_s[device], 1, 0)

    get_x.wait()
    for i in range(4):
        mix_s[i, :256, :] = x_s[i * 256 : (i + 1) * 256, :].astype(jnp.float32) + term(0, i)
    for n in range(1, 8):
        if n == 4:
            last_landed(6)
            last(7).start()
        if n % 2:
            last_landed(n)
        for i in range(4):
            if i % 2 == 0:
                result_landed(n, i // 2)
            if n < 7:
                mix_s[i, :256, :] += term(n, i)
            else:
                y_ref[i * 256 : (i + 1) * 256, :] = (mix_s[i, :256, :] + term(n, i)).astype(jnp.bfloat16)

    state(8).wait_send()
    for n in range(1, 8):
        state(n).wait_send()
        last(n).wait_send()
        for m in range(3):
            weight(n, m).wait_send()
    for step in range(1, 8):
        for half in range(2):
            result((me + step) % 8, half).wait_send()


def attended(x, gain, wq, wk, wv, wo):
    hbm, vmem = pl.BlockSpec(memory_space=pl.ANY), pl.BlockSpec(memory_space=pltpu.VMEM)
    dma = pltpu.SemaphoreType.DMA
    low = jnp.bfloat16
    return pl.pallas_call(
        _body,
        in_specs=[hbm] * 10,
        out_specs=[hbm, vmem],
        out_shape=[jax.ShapeDtypeStruct((8, OWN, DEPTH), low), pltpu.VMEM((OWN, DEPTH), low)],
        scratch_shapes=[pltpu.VMEM((DEPTH,), low), pltpu.VMEM((OWN, HALF), jnp.float32), pltpu.VMEM((OWN, HALF), jnp.float32),
                        pltpu.VMEM((8, HALF), jnp.float32), pltpu.VMEM((8, HALF), jnp.float32),
                        pltpu.VMEM((OWN, DEPTH), low), pltpu.VMEM((OWN, DEPTH), low), pltpu.VMEM((DEPTH, 3 * HEAD), low), pltpu.VMEM((8, HEAD, DEPTH), low),
                        pltpu.VMEM((8, OWN, HEAD), low),
                        pltpu.VMEM((8 * OWN, HEAD), low), pltpu.VMEM((8 * OWN, HEAD), low), pltpu.VMEM((TALL, 8 * OWN), low),
                        pltpu.VMEM((4, 8, CHUNK), jnp.float32), pltpu.VMEM((4, TALL, CHUNK), jnp.float32), pltpu.VMEM((8 * OWN, HEAD), low),
                        dma((11,)), dma((24,)), dma((24,)), dma((9,)), dma((9,)), dma((8,)), dma((8,)), dma((16,)), dma((16,))],
        compiler_params=pltpu.CompilerParams(collective_id=0, has_side_effects=True, vmem_limit_bytes=VMEM),
        cost_estimate=pl.CostEstimate(flops=2**36, transcendentals=2**25, bytes_accessed=2**27),
        name="attended",
    )(x, gain, wq, wk, wv, wo, *(jnp.asarray(t) for t in tables()))


def solution(mesh):
    def step(x, gain, wq, wk, wv, wo):
        return attended(x, gain, wq, wk, wv, wo)[1]

    tokens, whole = P(("dp", "sp"), None), P("sp", None)
    return jax.shard_map(
        step,
        mesh=mesh,
        in_specs=(tokens, P(None), whole, whole, whole, whole),
        out_specs=tokens,
        check_vma=False,
    )
```

```python
import functools

import jax
import jax.numpy as jnp
import numpy as np
from jax import lax
from jax.experimental import pallas as pl
from jax.experimental.pallas import tpu as pltpu
from jax.sharding import PartitionSpec as P

NEG = -1e30
LOG2E = 1.4426950408889634
HEAD = 256
HALF = HEAD // 2
THETA = 10000
VMEM = 58 * 2**20
STRIP = 512
KEYS = 512
OWN = 1024
CUT = 768
CHUNK = 2048
DEPTH = 2048
TALL = HEAD + 16
MESH = pl.DeviceIdType.MESH


def _dot(a, b, ca, cb):
    return lax.dot_general(a, b, (((ca,), (cb,)), ((), ())), preferred_element_type=jnp.float32)


def tables():
    rate = float(THETA) ** (-np.arange(HALF) / HALF)
    fine, coarse = np.arange(OWN)[:, None] * rate, OWN * np.arange(8)[:, None] * rate
    return [f(t).astype(np.float32) for t in (fine, coarse) for f in (np.cos, np.sin)]


def _body(x_ref, gain_in, wq_ref, wk_ref, wv_ref, wo_ref, cos_in, sin_in, cos8_in, sin8_in,
          piece_ref, y_ref,
          gain_ref, cos_ref, sin_ref, cos8_ref, sin8_ref, a_s, x_s, w_s, wo_s, seen_s, q_s, k_s, vt_s, top_s, mix_s, o_s,
          local, w_send, w_recv, p_send, p_recv, f_send, f_recv, o_send, o_recv):
    me = lax.axis_index("sp")
    x, y, core = me // 4, (me // 2) % 2, me % 2
    chip = me // 2
    late = 3 - chip

    def place(n):
        g, k = n // 2, (core + n) % 2
        along_x = jnp.where(g == 1, 1 - k, jnp.where(g == 2, k, jnp.where(g == 3, 1, 0)))
        along_y = jnp.where(g == 1, k, jnp.where(g == 2, 1 - k, jnp.where(g == 3, 1, 0)))
        return 4 * ((x + along_x) % 2) + 2 * ((y + along_y) % 2) + k

    partner, first, second = place(1), place(2), place(4)

    def to(device):
        return {"sp": device}

    def part(ref, n, all_ref):
        if n not in ((2, 8) if all_ref is piece_ref else (2, 8, 6, 9)):
            return ref
        cut, size = (CUT, OWN) if all_ref is piece_ref else (HALF, HEAD)
        return ref.at[pl.ds(0, cut)] if n in (2, 6) else ref.at[pl.ds(cut, size - cut)]

    def hop(n, own, all_ref, send, recv):
        first_hand = n in (1, 2, 4, 8)
        carried = me if first_hand else place({3: 2, 5: 4, 6: 2, 7: 6, 9: 2}[n])
        source = own if first_hand else all_ref.at[carried]
        target = first if n in (2, 8) else second if n in (4, 6, 9) else partner
        return pltpu.make_async_remote_copy(part(source, n, all_ref), part(all_ref.at[carried], n, all_ref), send.at[n], recv.at[n],
                                            device_id=to(target), device_id_type=MESH)

    def landed(n, own, all_ref, send, recv):
        pltpu.make_async_remote_copy(part(own, n, all_ref), part(all_ref.at[place({8: 2, 9: 6}.get(n, n))], n, all_ref), send.at[n], recv.at[n],
                                     device_id=to(partner), device_id_type=MESH).wait_recv()

    state = functools.partial(hop, own=a_s, all_ref=piece_ref, send=p_send, recv=p_recv)
    state_landed = functools.partial(landed, own=a_s, all_ref=piece_ref, send=p_send, recv=p_recv)
    last = functools.partial(hop, own=wo_ref, all_ref=wo_s, send=f_send, recv=f_recv)
    last_landed = functools.partial(landed, own=wo_ref, all_ref=wo_s, send=f_send, recv=f_recv)

    get_x = pltpu.make_async_copy(x_ref, x_s, local.at[0])
    get_wo = pltpu.make_async_copy(wo_ref, wo_s.at[me], local.at[1])
    get_tables = [pltpu.make_async_copy(cos_in, cos_ref, local.at[6]), pltpu.make_async_copy(sin_in, sin_ref, local.at[7]),
                  pltpu.make_async_copy(cos8_in, cos8_ref, local.at[8]), pltpu.make_async_copy(sin8_in, sin8_ref, local.at[9])]
    get_gain = pltpu.make_async_copy(gain_in, gain_ref, local.at[10])
    get_x.start()
    get_gain.start()

    barrier = pltpu.get_barrier_semaphore()
    for step in range(1, 8):
        pl.semaphore_signal(barrier, inc=1, device_id=to((me + step) % 8), device_id_type=MESH)
    pl.semaphore_wait(barrier, 7)

    weights = (wq_ref, wk_ref, wv_ref)

    def columns(m, device):
        return weights[m].at[:, pl.ds(pl.multiple_of(device * HEAD, HEAD), HEAD)]

    def rows(m, device):
        return w_s.at[pl.ds(pl.multiple_of(device * HEAD, HEAD), HEAD), pl.ds(m * HEAD, HEAD)]

    def weight(n, m):
        k = (core + n) % 2
        g, base = n // 2, core
        flip_x = (1 - base if g == 1 else base if g == 2 else 1) if g else 0
        flip_y = (base if g == 1 else 1 - base if g == 2 else 1) if g else 0
        device = 4 * ((x + flip_x) % 2) + 2 * ((y + flip_y) % 2) + k
        return pltpu.make_async_remote_copy(columns(m, device), rows(m, me), w_send.at[3 * n + m], w_recv.at[3 * n + m], device_id=to(device),
                                            device_id_type=MESH)

    for n in (6, 7, 2, 5, 4, 3, 1):
        for m in range(3):
            weight(n, m).start()
    mine = [pltpu.make_async_copy(columns(m, me), rows(m, me), local.at[2 + m]) for m in range(3)]
    for copy in mine:
        copy.start()

    for copy in (get_wo, *get_tables):
        copy.start()
    get_x.wait()
    get_gain.wait()

    def norm(i, _):
        at = pl.ds(pl.multiple_of(i * 128, 128), 128)
        wide = x_s[at, :].astype(jnp.float32)
        scale = lax.rsqrt(jnp.mean(wide * wide, -1, keepdims=True) + 1e-6)
        a_s[at, :] = (wide * scale * gain_ref[...].astype(jnp.float32)).astype(jnp.bfloat16)

    lax.fori_loop(0, OWN // 128, norm, None)
    state(2).start()
    state(8).start()
    state(1).start()

    top_s[...] = jnp.full(top_s.shape, NEG, jnp.float32)

    def clear(i, _):
        mix_s[i] = jnp.zeros(mix_s.shape[1:], jnp.float32)

    lax.fori_loop(0, 4, clear, None)
    vt_s[HEAD:, :] = jnp.ones((TALL - HEAD, vt_s.shape[1]), jnp.bfloat16)
    for copy in (*mine, *get_tables):
        copy.wait()
    for n in range(1, 8):
        for m in range(3):
            pltpu.make_async_remote_copy(columns(m, me), rows(m, place(n)), w_send.at[3 * n + m], w_recv.at[3 * n + m], device_id=to(partner),
                                         device_id_type=MESH).wait_recv()

    def project(source, piece):
        cos8, sin8 = cos8_ref[pl.ds(piece, 1), :], sin8_ref[pl.ds(piece, 1), :]

        def tile(i, _):
            at = pl.ds(pl.multiple_of(i * 256, 256), 256)
            into = pl.ds(pl.multiple_of(piece * OWN + i * 256, 256), 256)
            total = _dot(source[at, :], w_s[...], 1, 0).astype(jnp.bfloat16)
            fine_cos, fine_sin = cos_ref[at, :], sin_ref[at, :]
            cos, sin = fine_cos * cos8 - fine_sin * sin8, fine_sin * cos8 + fine_cos * sin8
            for ref, column in ((q_s, 0), (k_s, HEAD)):
                one, two = total[:, column : column + HALF].astype(jnp.float32), total[:, column + HALF : column + HEAD].astype(jnp.float32)
                ref[into, :HALF] = (one * cos - two * sin).astype(jnp.bfloat16)
                ref[into, HALF:] = (two * cos + one * sin).astype(jnp.bfloat16)
            vt_s[:HEAD, into] = total[:, 2 * HEAD :].T

        lax.fori_loop(0, OWN // 256, tile, None)

    e = HEAD**-0.5 * LOG2E
    strips, blocks = CHUNK // STRIP, CHUNK // KEYS

    def block(qi, ki, j, from_strip, diagonal):
        here = pl.ds(pl.multiple_of(ki * CHUNK + j * KEYS, KEYS), KEYS)
        keys, values = k_s[here, :], vt_s[:, here]
        mine = [slice(n * STRIP, (n + 1) * STRIP) for n in range(from_strip, strips)]
        scores = [_dot(keys, q_s[pl.ds(pl.multiple_of(qi * CHUNK + at.start, STRIP), STRIP), :], 1, 1) for at in mine]
        weights, keeps = [], []
        for n, (at, s) in enumerate(zip(mine, scores)):
            if diagonal and n == 0:
                s = jnp.where(lax.broadcasted_iota(jnp.int32, s.shape, 1) >= lax.broadcasted_iota(jnp.int32, s.shape, 0), s, 2 * NEG)
            old = top_s[qi, 0:1, at]
            top = jnp.maximum(old, s.max(axis=0, keepdims=True))
            top_s[qi, 0:1, at] = top
            weights.append(jnp.exp2((s - top) * e).astype(jnp.bfloat16))
            keeps.append(jnp.exp2((old - top) * e))
        for at, p, keep in zip(mine, weights, keeps):
            mix_s[qi, :, at] = mix_s[qi, :, at] * keep + _dot(values, p, 1, 0)

    def pair(qi, ki):
        @pl.when(qi != ki)
        def _():
            lax.fori_loop(0, blocks, lambda j, _: block(qi, ki, j, 0, False), None)

        @pl.when(qi == ki)
        def _():
            for j in range(blocks):
                block(qi, ki, j, j, True)

    def result(device, half):
        rows = o_s.at[pl.ds(pl.multiple_of(device * OWN + half * 512, 512), 512), :]
        return pltpu.make_async_remote_copy(rows, seen_s.at[me, pl.ds(half * 512, 512)], o_send.at[2 * device + half], o_recv.at[2 * me + half],
                                            device_id=to(device), device_id_type=MESH)

    def send(device):
        for half in range(2):
            result(device, half).start()

    def own_result():
        return pltpu.make_async_copy(o_s.at[pl.ds(pl.multiple_of(me * OWN, OWN), OWN), :], seen_s.at[me], local.at[0])

    def finished(qi):
        for n in range(strips):
            at = slice(n * STRIP, (n + 1) * STRIP)
            o_s[pl.ds(pl.multiple_of(qi * CHUNK + at.start, STRIP), STRIP), :] = (
                mix_s[qi, :HEAD, at] * (1 / mix_s[qi, HEAD : HEAD + 1, at])).T.astype(jnp.bfloat16)

    def keep(qi):
        @pl.when(qi == chip)
        def _():
            own_result().start()
            send(partner)

    def early(qi, _):
        finished(qi)
        keep(qi)

        @pl.when(qi != chip)
        def _():
            send(2 * qi + core)
            send(2 * qi + 1 - core)

    near = [jnp.where(late > n, n, n + 1) for n in range(3)]

    table = (((2, 0, 1), (1, 0, 1), (0, 0, 1), (3, 0, 1)), ((3, 1, 1), (1, 1, 0), (1, 0, 1), (2, 1, 1)),
             ((3, 2, 1), (2, 2, 0), (2, 0, 0), (2, 1, 1)), ((3, 3, 0), (3, 0, 0), (3, 1, 0), (3, 2, 1)))

    def far(t):
        def pick(values, index):
            return jnp.where(index == 0, values[0], jnp.where(index == 1, values[1], jnp.where(index == 2, values[2], values[3])))

        return [pick([pick([entry[part] for entry in row], t - 6) for row in table], late) for part in range(3)]

    def chunks(t):
        qi = jnp.where(t == 0, chip, jnp.where(t == 1, (chip + 2) % 4, jnp.where(t == 2, chip + 1 - 2 * (chip % 2), jnp.where(t == 3, near[1], near[2]))))
        ki = jnp.where(t < 3, qi, jnp.where(t == 5, near[1], near[0]))
        far_q, far_k, _ = far(t)
        return jnp.where(t < 6, qi, far_q), jnp.where(t < 6, ki, far_k)

    def stage(n, _):
        @pl.when(n == 1)
        def _():
            state_landed(1)

        @pl.when(n == 2)
        def _():
            state_landed(2)
            state(4).start()
            state_landed(8)
            state(6).start()
            state(3).start()
            last(4).start()

        @pl.when(n == 3)
        def _():
            state_landed(3)

        @pl.when(n == 4)
        def _():
            state_landed(4)
            state(5).start()

        @pl.when(n == 5)
        def _():
            state_landed(5)

        @pl.when(n == 6)
        def _():
            state_landed(6)
            state(7).start()
            last(2).start()
            last(8).start()
            last(1).start()
            lax.fori_loop(0, late, early, None)

        @pl.when(n == 7)
        def _():
            state_landed(7)

        piece = place(n)

        @pl.when(n > 0)
        def _():
            copy = pltpu.make_async_copy(piece_ref.at[piece], x_s, local.at[5])
            copy.start()
            copy.wait()
            project(x_s, piece)

        @pl.when(n == 0)
        def _():
            project(a_s, piece)

        def step(t, _):
            @pl.when(t == 8)
            def _():
                last_landed(4)
                last(5).start()

            @pl.when(t == 6)
            def _():
                last_landed(2)
                last(6).start()

            @pl.when(t == 7)
            def _():
                last_landed(8)
                last(9).start()
                last(3).start()

            qi, ki = chunks(t)
            pair(qi, ki)


            @pl.when((t > 5) & (far(t)[2] == 1))
            def _():
                finished(qi)
                keep(qi)

                @pl.when(qi != chip)
                def _():
                    send(2 * qi + core)
                    send(2 * qi + 1 - core)

        start = jnp.where(n == 5, 1, jnp.where(n == 7, 6, 0))
        stop = jnp.where(n == 3, 1, jnp.where(n == 5, 6, jnp.where(n == 7, 10, 0)))
        lax.fori_loop(start, stop, step, None)

    lax.fori_loop(0, 8, stage, None)

    get_x = pltpu.make_async_copy(x_ref, x_s, local.at[2])
    get_x.start()
    get_wo.wait()
    own_result().wait()

    def result_landed(n, half):
        device = place(n)
        pltpu.make_async_remote_copy(o_s.at[pl.ds(0, 512), :], seen_s.at[device, pl.ds(half * 512, 512)], o_send.at[2 * device + half],
                                     o_recv.at[2 * device + half], device_id=to(partner), device_id_type=MESH).wait_recv()

    def term(n, i):
        device = place(n)
        return _dot(seen_s[device, i * 256 : (i + 1) * 256, :], wo_s[device], 1, 0)

    get_x.wait()
    for i in range(4):
        mix_s[i, :256, :] = x_s[i * 256 : (i + 1) * 256, :].astype(jnp.float32) + term(0, i)
    for n in range(1, 8):
        if n == 4:
            last_landed(6)
            last_landed(9)
            last(7).start()
        if n % 2:
            last_landed(n)
        for i in range(4):
            if i % 2 == 0:
                result_landed(n, i // 2)
            if n < 7:
                mix_s[i, :256, :] += term(n, i)
            else:
                y_ref[i * 256 : (i + 1) * 256, :] = (mix_s[i, :256, :] + term(n, i)).astype(jnp.bfloat16)

    state(8).wait_send()
    last(8).wait_send()
    last(9).wait_send()
    for n in range(1, 8):
        state(n).wait_send()
        last(n).wait_send()
        for m in range(3):
            weight(n, m).wait_send()
    for step in range(1, 8):
        for half in range(2):
            result((me + step) % 8, half).wait_send()


def attended(x, gain, wq, wk, wv, wo):
    hbm, vmem = pl.BlockSpec(memory_space=pl.ANY), pl.BlockSpec(memory_space=pltpu.VMEM)
    dma = pltpu.SemaphoreType.DMA
    low = jnp.bfloat16
    return pl.pallas_call(
        _body,
        in_specs=[hbm] * 10,
        out_specs=[hbm, vmem],
        out_shape=[jax.ShapeDtypeStruct((8, OWN, DEPTH), low), pltpu.VMEM((OWN, DEPTH), low)],
        scratch_shapes=[pltpu.VMEM((DEPTH,), low), pltpu.VMEM((OWN, HALF), jnp.float32), pltpu.VMEM((OWN, HALF), jnp.float32),
                        pltpu.VMEM((8, HALF), jnp.float32), pltpu.VMEM((8, HALF), jnp.float32),
                        pltpu.VMEM((OWN, DEPTH), low), pltpu.VMEM((OWN, DEPTH), low), pltpu.VMEM((DEPTH, 3 * HEAD), low), pltpu.VMEM((8, HEAD, DEPTH), low),
                        pltpu.VMEM((8, OWN, HEAD), low),
                        pltpu.VMEM((8 * OWN, HEAD), low), pltpu.VMEM((8 * OWN, HEAD), low), pltpu.VMEM((TALL, 8 * OWN), low),
                        pltpu.VMEM((4, 8, CHUNK), jnp.float32), pltpu.VMEM((4, TALL, CHUNK), jnp.float32), pltpu.VMEM((8 * OWN, HEAD), low),
                        dma((11,)), dma((24,)), dma((24,)), dma((9,)), dma((9,)), dma((10,)), dma((10,)), dma((16,)), dma((16,))],
        compiler_params=pltpu.CompilerParams(collective_id=0, has_side_effects=True, vmem_limit_bytes=VMEM),
        cost_estimate=pl.CostEstimate(flops=2**36, transcendentals=2**25, bytes_accessed=2**27),
        name="attended",
    )(x, gain, wq, wk, wv, wo, *(jnp.asarray(t) for t in tables()))


def solution(mesh):
    def step(x, gain, wq, wk, wv, wo):
        return attended(x, gain, wq, wk, wv, wo)[1]

    tokens, whole = P(("dp", "sp"), None), P("sp", None)
    return jax.shard_map(
        step,
        mesh=mesh,
        in_specs=(tokens, P(None), whole, whole, whole, whole),
        out_specs=tokens,
        check_vma=False,
    )
```

```python
import functools

import jax
import jax.numpy as jnp
import numpy as np
from jax import lax
from jax.experimental import pallas as pl
from jax.experimental.pallas import tpu as pltpu
from jax.sharding import PartitionSpec as P

NEG = -1e30
LOG2E = 1.4426950408889634
HEAD = 256
HALF = HEAD // 2
THETA = 10000
VMEM = 58 * 2**20
STRIP = 512
KEYS = 512
OWN = 1024
CUT = 768
LAST_CUT = 896
CHUNK = 2048
DEPTH = 2048
TALL = HEAD + 16
MESH = pl.DeviceIdType.MESH


def _dot(a, b, ca, cb):
    return lax.dot_general(a, b, (((ca,), (cb,)), ((), ())), preferred_element_type=jnp.float32)


def tables():
    rate = float(THETA) ** (-np.arange(HALF) / HALF)
    fine, coarse = np.arange(OWN)[:, None] * rate, OWN * np.arange(8)[:, None] * rate
    return [f(t).astype(np.float32) for t in (fine, coarse) for f in (np.cos, np.sin)]


def _body(x_ref, gain_in, wq_ref, wk_ref, wv_ref, wo_ref, cos_in, sin_in, cos8_in, sin8_in,
          piece_ref, y_ref,
          gain_ref, cos_ref, sin_ref, cos8_ref, sin8_ref, a_s, x_s, w_s, wo_s, seen_s, q_s, k_s, vt_s, top_s, mix_s, o_s,
          local, w_send, w_recv, p_send, p_recv, f_send, f_recv, o_send, o_recv):
    me = lax.axis_index("sp")
    x, y, core = me // 4, (me // 2) % 2, me % 2
    chip = me // 2
    late = 3 - chip

    def place(n):
        g, k = n // 2, (core + n) % 2
        along_x = jnp.where(g == 1, 1 - k, jnp.where(g == 2, k, jnp.where(g == 3, 1, 0)))
        along_y = jnp.where(g == 1, k, jnp.where(g == 2, 1 - k, jnp.where(g == 3, 1, 0)))
        return 4 * ((x + along_x) % 2) + 2 * ((y + along_y) % 2) + k

    partner, first, second = place(1), place(2), place(4)

    def to(device):
        return {"sp": device}

    def part(ref, n, all_ref):
        if n not in (2, 8, 6, 9):
            return ref
        cut, size = ((CUT if n in (2, 8) else LAST_CUT), OWN) if all_ref is piece_ref else (HALF, HEAD)
        return ref.at[pl.ds(0, cut)] if n in (2, 6) else ref.at[pl.ds(cut, size - cut)]

    def hop(n, own, all_ref, send, recv):
        first_hand = n in (1, 2, 4, 8)
        carried = me if first_hand else place({3: 2, 5: 4, 6: 2, 7: 6, 9: 2}[n])
        source = own if first_hand else all_ref.at[carried]
        target = first if n in (2, 8) else second if n in (4, 6, 9) else partner
        return pltpu.make_async_remote_copy(part(source, n, all_ref), part(all_ref.at[carried], n, all_ref), send.at[n], recv.at[n],
                                            device_id=to(target), device_id_type=MESH)

    def landed(n, own, all_ref, send, recv):
        pltpu.make_async_remote_copy(part(own, n, all_ref), part(all_ref.at[place({8: 2, 9: 6}.get(n, n))], n, all_ref), send.at[n], recv.at[n],
                                     device_id=to(partner), device_id_type=MESH).wait_recv()

    state = functools.partial(hop, own=a_s, all_ref=piece_ref, send=p_send, recv=p_recv)
    state_landed = functools.partial(landed, own=a_s, all_ref=piece_ref, send=p_send, recv=p_recv)
    last = functools.partial(hop, own=wo_ref, all_ref=wo_s, send=f_send, recv=f_recv)
    last_landed = functools.partial(landed, own=wo_ref, all_ref=wo_s, send=f_send, recv=f_recv)

    get_x = pltpu.make_async_copy(x_ref, x_s, local.at[0])
    get_wo = pltpu.make_async_copy(wo_ref, wo_s.at[me], local.at[1])
    get_tables = [pltpu.make_async_copy(cos_in, cos_ref, local.at[6]), pltpu.make_async_copy(sin_in, sin_ref, local.at[7]),
                  pltpu.make_async_copy(cos8_in, cos8_ref, local.at[8]), pltpu.make_async_copy(sin8_in, sin8_ref, local.at[9])]
    get_gain = pltpu.make_async_copy(gain_in, gain_ref, local.at[10])
    get_x.start()
    get_gain.start()

    barrier = pltpu.get_barrier_semaphore()
    for step in range(1, 8):
        pl.semaphore_signal(barrier, inc=1, device_id=to((me + step) % 8), device_id_type=MESH)
    pl.semaphore_wait(barrier, 7)

    weights = (wq_ref, wk_ref, wv_ref)

    def columns(m, device):
        return weights[m].at[:, pl.ds(pl.multiple_of(device * HEAD, HEAD), HEAD)]

    def rows(m, device):
        return w_s.at[pl.ds(pl.multiple_of(device * HEAD, HEAD), HEAD), pl.ds(m * HEAD, HEAD)]

    def weight(n, m):
        k = (core + n) % 2
        g, base = n // 2, core
        flip_x = (1 - base if g == 1 else base if g == 2 else 1) if g else 0
        flip_y = (base if g == 1 else 1 - base if g == 2 else 1) if g else 0
        device = 4 * ((x + flip_x) % 2) + 2 * ((y + flip_y) % 2) + k
        return pltpu.make_async_remote_copy(columns(m, device), rows(m, me), w_send.at[3 * n + m], w_recv.at[3 * n + m], device_id=to(device),
                                            device_id_type=MESH)

    for n in (6, 7, 2, 5, 4, 3, 1):
        for m in range(3):
            weight(n, m).start()
    mine = [pltpu.make_async_copy(columns(m, me), rows(m, me), local.at[2 + m]) for m in range(3)]
    for copy in mine:
        copy.start()

    for copy in (get_wo, *get_tables):
        copy.start()
    get_x.wait()
    get_gain.wait()

    def norm(i, _):
        at = pl.ds(pl.multiple_of(i * 128, 128), 128)
        wide = x_s[at, :].astype(jnp.float32)
        scale = lax.rsqrt(jnp.mean(wide * wide, -1, keepdims=True) + 1e-6)
        a_s[at, :] = (wide * scale * gain_ref[...].astype(jnp.float32)).astype(jnp.bfloat16)

    lax.fori_loop(0, OWN // 128, norm, None)
    state(2).start()
    state(8).start()
    state(1).start()

    top_s[...] = jnp.full(top_s.shape, NEG, jnp.float32)

    def clear(i, _):
        mix_s[i] = jnp.zeros(mix_s.shape[1:], jnp.float32)

    lax.fori_loop(0, 4, clear, None)
    vt_s[HEAD:, :] = jnp.ones((TALL - HEAD, vt_s.shape[1]), jnp.bfloat16)
    for copy in (*mine, *get_tables):
        copy.wait()
    for n in range(1, 8):
        for m in range(3):
            pltpu.make_async_remote_copy(columns(m, me), rows(m, place(n)), w_send.at[3 * n + m], w_recv.at[3 * n + m], device_id=to(partner),
                                         device_id_type=MESH).wait_recv()

    def project(source, piece):
        cos8, sin8 = cos8_ref[pl.ds(piece, 1), :], sin8_ref[pl.ds(piece, 1), :]

        def tile(i, _):
            at = pl.ds(pl.multiple_of(i * 256, 256), 256)
            into = pl.ds(pl.multiple_of(piece * OWN + i * 256, 256), 256)
            total = _dot(source[at, :], w_s[...], 1, 0).astype(jnp.bfloat16)
            fine_cos, fine_sin = cos_ref[at, :], sin_ref[at, :]
            cos, sin = fine_cos * cos8 - fine_sin * sin8, fine_sin * cos8 + fine_cos * sin8
            for ref, column in ((q_s, 0), (k_s, HEAD)):
                one, two = total[:, column : column + HALF].astype(jnp.float32), total[:, column + HALF : column + HEAD].astype(jnp.float32)
                ref[into, :HALF] = (one * cos - two * sin).astype(jnp.bfloat16)
                ref[into, HALF:] = (two * cos + one * sin).astype(jnp.bfloat16)
            vt_s[:HEAD, into] = total[:, 2 * HEAD :].T

        lax.fori_loop(0, OWN // 256, tile, None)

    e = HEAD**-0.5 * LOG2E
    strips, blocks = CHUNK // STRIP, CHUNK // KEYS

    def block(qi, ki, j, from_strip, diagonal):
        here = pl.ds(pl.multiple_of(ki * CHUNK + j * KEYS, KEYS), KEYS)
        keys, values = k_s[here, :], vt_s[:, here]
        mine = [slice(n * STRIP, (n + 1) * STRIP) for n in range(from_strip, strips)]
        scores = [_dot(keys, q_s[pl.ds(pl.multiple_of(qi * CHUNK + at.start, STRIP), STRIP), :], 1, 1) for at in mine]
        weights, keeps = [], []
        for n, (at, s) in enumerate(zip(mine, scores)):
            if diagonal and n == 0:
                s = jnp.where(lax.broadcasted_iota(jnp.int32, s.shape, 1) >= lax.broadcasted_iota(jnp.int32, s.shape, 0), s, 2 * NEG)
            old = top_s[qi, 0:1, at]
            top = jnp.maximum(old, s.max(axis=0, keepdims=True))
            top_s[qi, 0:1, at] = top
            weights.append(jnp.exp2((s - top) * e).astype(jnp.bfloat16))
            keeps.append(jnp.exp2((old - top) * e))
        for at, p, keep in zip(mine, weights, keeps):
            mix_s[qi, :, at] = mix_s[qi, :, at] * keep + _dot(values, p, 1, 0)

    def pair(qi, ki):
        @pl.when(qi != ki)
        def _():
            lax.fori_loop(0, blocks, lambda j, _: block(qi, ki, j, 0, False), None)

        @pl.when(qi == ki)
        def _():
            for j in range(blocks):
                block(qi, ki, j, j, True)

    def result(device, half):
        rows = o_s.at[pl.ds(pl.multiple_of(device * OWN + half * 512, 512), 512), :]
        return pltpu.make_async_remote_copy(rows, seen_s.at[me, pl.ds(half * 512, 512)], o_send.at[2 * device + half], o_recv.at[2 * me + half],
                                            device_id=to(device), device_id_type=MESH)

    def send(device):
        for half in range(2):
            result(device, half).start()

    def own_result():
        return pltpu.make_async_copy(o_s.at[pl.ds(pl.multiple_of(me * OWN, OWN), OWN), :], seen_s.at[me], local.at[0])

    def finished(qi):
        for n in range(strips):
            at = slice(n * STRIP, (n + 1) * STRIP)
            o_s[pl.ds(pl.multiple_of(qi * CHUNK + at.start, STRIP), STRIP), :] = (
                mix_s[qi, :HEAD, at] * (1 / mix_s[qi, HEAD : HEAD + 1, at])).T.astype(jnp.bfloat16)

    def keep(qi):
        @pl.when(qi == chip)
        def _():
            own_result().start()
            send(partner)

    def early(qi, _):
        finished(qi)
        keep(qi)

        @pl.when(qi != chip)
        def _():
            send(2 * qi + core)
            send(2 * qi + 1 - core)

    near = [jnp.where(late > n, n, n + 1) for n in range(3)]

    table = (((2, 0, 1), (1, 0, 1), (0, 0, 1), (3, 0, 1)), ((3, 1, 1), (1, 1, 0), (1, 0, 1), (2, 1, 1)),
             ((3, 2, 1), (2, 2, 0), (2, 0, 0), (2, 1, 1)), ((3, 3, 0), (3, 0, 0), (3, 1, 0), (3, 2, 1)))

    def far(t):
        def pick(values, index):
            return jnp.where(index == 0, values[0], jnp.where(index == 1, values[1], jnp.where(index == 2, values[2], values[3])))

        return [pick([pick([entry[part] for entry in row], t - 6) for row in table], late) for part in range(3)]

    def chunks(t):
        qi = jnp.where(t == 0, chip, jnp.where(t == 1, (chip + 2) % 4, jnp.where(t == 2, chip + 1 - 2 * (chip % 2), jnp.where(t == 3, near[1], near[2]))))
        ki = jnp.where(t < 3, qi, jnp.where(t == 5, near[1], near[0]))
        far_q, far_k, _ = far(t)
        return jnp.where(t < 6, qi, far_q), jnp.where(t < 6, ki, far_k)

    def stage(n, _):
        @pl.when(n == 1)
        def _():
            state_landed(1)

        @pl.when(n == 2)
        def _():
            state_landed(2)
            state(4).start()
            state_landed(8)
            state(6).start()
            state(9).start()
            state(3).start()
            last(4).start()

        @pl.when(n == 3)
        def _():
            state_landed(3)

        @pl.when(n == 4)
        def _():
            state_landed(4)
            state(5).start()

        @pl.when(n == 5)
        def _():
            state_landed(5)

        @pl.when(n == 6)
        def _():
            state_landed(6)
            last(2).start()
            last(8).start()
            state_landed(9)
            state(7).start()
            last(1).start()
            lax.fori_loop(0, late, early, None)

        @pl.when(n == 7)
        def _():
            state_landed(7)

        piece = place(n)

        @pl.when(n > 0)
        def _():
            copy = pltpu.make_async_copy(piece_ref.at[piece], x_s, local.at[5])
            copy.start()
            copy.wait()
            project(x_s, piece)

        @pl.when(n == 0)
        def _():
            project(a_s, piece)

        def step(t, _):
            @pl.when(t == 8)
            def _():
                last_landed(4)
                last(5).start()

            @pl.when(t == 6)
            def _():
                last_landed(2)
                last(6).start()

            @pl.when(t == 7)
            def _():
                last_landed(8)
                last(9).start()
                last(3).start()

            qi, ki = chunks(t)
            pair(qi, ki)


            @pl.when((t > 5) & (far(t)[2] == 1))
            def _():
                finished(qi)
                keep(qi)

                @pl.when(qi != chip)
                def _():
                    send(2 * qi + core)
                    send(2 * qi + 1 - core)

        start = jnp.where(n == 5, 1, jnp.where(n == 7, 6, 0))
        stop = jnp.where(n == 3, 1, jnp.where(n == 5, 6, jnp.where(n == 7, 10, 0)))
        lax.fori_loop(start, stop, step, None)

    lax.fori_loop(0, 8, stage, None)

    get_x = pltpu.make_async_copy(x_ref, x_s, local.at[2])
    get_x.start()
    get_wo.wait()
    own_result().wait()

    def result_landed(n, half):
        device = place(n)
        pltpu.make_async_remote_copy(o_s.at[pl.ds(0, 512), :], seen_s.at[device, pl.ds(half * 512, 512)], o_send.at[2 * device + half],
                                     o_recv.at[2 * device + half], device_id=to(partner), device_id_type=MESH).wait_recv()

    def term(n, i):
        device = place(n)
        return _dot(seen_s[device, i * 256 : (i + 1) * 256, :], wo_s[device], 1, 0)

    get_x.wait()
    for i in range(4):
        mix_s[i, :256, :] = x_s[i * 256 : (i + 1) * 256, :].astype(jnp.float32) + term(0, i)
    for n in range(1, 8):
        if n == 4:
            last_landed(6)
            last_landed(9)
            last(7).start()
        if n % 2:
            last_landed(n)
        for i in range(4):
            if i % 2 == 0:
                result_landed(n, i // 2)
            if n < 7:
                mix_s[i, :256, :] += term(n, i)
            else:
                y_ref[i * 256 : (i + 1) * 256, :] = (mix_s[i, :256, :] + term(n, i)).astype(jnp.bfloat16)

    state(8).wait_send()
    state(9).wait_send()
    last(8).wait_send()
    last(9).wait_send()
    for n in range(1, 8):
        state(n).wait_send()
        last(n).wait_send()
        for m in range(3):
            weight(n, m).wait_send()
    for step in range(1, 8):
        for half in range(2):
            result((me + step) % 8, half).wait_send()


def attended(x, gain, wq, wk, wv, wo):
    hbm, vmem = pl.BlockSpec(memory_space=pl.ANY), pl.BlockSpec(memory_space=pltpu.VMEM)
    dma = pltpu.SemaphoreType.DMA
    low = jnp.bfloat16
    return pl.pallas_call(
        _body,
        in_specs=[hbm] * 10,
        out_specs=[hbm, vmem],
        out_shape=[jax.ShapeDtypeStruct((8, OWN, DEPTH), low), pltpu.VMEM((OWN, DEPTH), low)],
        scratch_shapes=[pltpu.VMEM((DEPTH,), low), pltpu.VMEM((OWN, HALF), jnp.float32), pltpu.VMEM((OWN, HALF), jnp.float32),
                        pltpu.VMEM((8, HALF), jnp.float32), pltpu.VMEM((8, HALF), jnp.float32),
                        pltpu.VMEM((OWN, DEPTH), low), pltpu.VMEM((OWN, DEPTH), low), pltpu.VMEM((DEPTH, 3 * HEAD), low), pltpu.VMEM((8, HEAD, DEPTH), low),
                        pltpu.VMEM((8, OWN, HEAD), low),
                        pltpu.VMEM((8 * OWN, HEAD), low), pltpu.VMEM((8 * OWN, HEAD), low), pltpu.VMEM((TALL, 8 * OWN), low),
                        pltpu.VMEM((4, 8, CHUNK), jnp.float32), pltpu.VMEM((4, TALL, CHUNK), jnp.float32), pltpu.VMEM((8 * OWN, HEAD), low),
                        dma((11,)), dma((24,)), dma((24,)), dma((10,)), dma((10,)), dma((10,)), dma((10,)), dma((16,)), dma((16,))],
        compiler_params=pltpu.CompilerParams(collective_id=0, has_side_effects=True, vmem_limit_bytes=VMEM),
        cost_estimate=pl.CostEstimate(flops=2**36, transcendentals=2**25, bytes_accessed=2**27),
        name="attended",
    )(x, gain, wq, wk, wv, wo, *(jnp.asarray(t) for t in tables()))


def solution(mesh):
    def step(x, gain, wq, wk, wv, wo):
        return attended(x, gain, wq, wk, wv, wo)[1]

    tokens, whole = P(("dp", "sp"), None), P("sp", None)
    return jax.shard_map(
        step,
        mesh=mesh,
        in_specs=(tokens, P(None), whole, whole, whole, whole),
        out_specs=tokens,
        check_vma=False,
    )
```
